32 devices in a mesh: rep: 2 (over x), seq: 8 (over z, y), tp: 2 (over core).
Axes of the slice: x: 2, y: 2, z: 4, core: 2. Of those that a mesh axis runs over, the one named last changes fastest.
Arguments:
- prefill_query: bfloat16 [8192, 2048], P(('rep', 'seq'), 'tp'), parts along dimension 0, may hold values from -50 to 50
- prefill_key: bfloat16 [8192, 512], P(('rep', 'seq'), 'tp'), parts along dimension 0, may hold values from -6 to 6
- prefill_value: bfloat16 [8192, 512], P(('rep', 'seq'), 'tp'), parts along dimension 0, may hold values from -6 to 6
- doc_ids: int32 [8192], P('rep'), parts along dimension 0, may hold values from 0 to 3, never falling along the last dimension, each value on 1 to 2048 neighbouring positions
- head_window: int32 [16], P('tp'), may hold values from 1024 to 4096, as said below
- dec_query: bfloat16 [128, 2048], P('rep', 'tp'), parts along dimension 0, may hold values from -50 to 50
- dec_key: bfloat16 [128, 512], P('rep', 'tp'), parts along dimension 0, may hold values from -6 to 6
- dec_value: bfloat16 [128, 512], P('rep', 'tp'), parts along dimension 0, may hold values from -6 to 6
- cache_key: bfloat16 [65536, 512], P(('rep', 'seq'), 'tp'), parts along dimension 0, may hold values from -6 to 6
- cache_value: bfloat16 [65536, 512], P(('rep', 'seq'), 'tp'), parts along dimension 0, may hold values from -6 to 6
- page_order: int32 [512], P(('rep', 'seq')), parts along dimension 0, may hold values from 0 to 255, each once
- lengths: int32 [128], P('rep'), parts along dimension 0, may hold values from 1 to 512, 16384 in all
- out_proj: bfloat16 [2048, 4096], P('tp'), may hold values from -0.125 to 0.125
Outputs:
- prompt_out: bfloat16 [8192, 4096], P(('rep', 'seq', 'tp')), parts along dimension 0
- decode_out: bfloat16 [128, 4096], P(('rep', 'tp')), parts along dimension 0
The draws below stay inside these ranges and needn't reach their ends.
There are 2 independent parts, one for each index of `rep`. The reference program is written for one: setup_inputs(seed, part) draws one part's arguments, and reference() takes and returns one part's arrays. A program takes and returns all parts, laid end to end along the dimension named above; an argument that names none is the same for every part. Nothing has to cross between parts.
Inputs may be any that keep to these rules, and one draw needn't show every extreme that they name: `head_window`: some head has window 4096.
All inputs are finite; a program needn't handle non-finite values.
Results may differ from the reference program's by a relative error of at most 0.015.
Values may be sent and summed in bfloat16 or wider, within the bound.
No kernel may reach another device: no remote copies, remote signals or barrier semaphores. Data moves between devices by JAX's collectives and lax.ppermute only.
A program may use at most 256 MiB of HBM per device.

```python
import math
import jax
import jax.numpy as jnp
import numpy as np
from jax import lax

D = 4096
HD = 128
HEADS = 16
KV_HEADS = 4
WINDOW = 4096
REQS = 64
PAGE = 128
TOKENS = 4096
PAGES = 256
MAXLEN = 512
N_TP = 2


def prompt_keys(key):
    base = jax.random.fold_in(key, 7)
    keys = jnp.clip(jax.random.normal(base, (TOKENS, KV_HEADS * HD), jnp.float32), -6.0, 6.0)
    return keys


def draw_prefill_key(key, part):
    return prompt_keys(key).astype(jnp.bfloat16)


def draw_prefill_query(key, part):
    base = jax.random.fold_in(key, 8)
    queries = jnp.clip(jax.random.normal(base, (TOKENS, HEADS * HD), jnp.float32), -6.0, 6.0)
    return queries.astype(jnp.bfloat16)


def decode_keys(key):
    base = jax.random.fold_in(key, 9)
    keys = jnp.clip(jax.random.normal(base, (REQS, KV_HEADS * HD), jnp.float32), -6.0, 6.0)
    return keys


def draw_dec_key(key, part):
    return decode_keys(key).astype(jnp.bfloat16)


def draw_dec_query(key, part):
    base = jax.random.fold_in(key, 10)
    queries = jnp.clip(jax.random.normal(base, (REQS, HEADS * HD), jnp.float32), -6.0, 6.0)
    return queries.astype(jnp.bfloat16)


def draw_head_window(key, part):
    widths = jax.random.randint(jax.random.fold_in(key, 3), (HEADS,), WINDOW // 4, WINDOW + 1)
    picked = jax.random.randint(jax.random.fold_in(key, 4), (), 0, HEADS)
    return jnp.where(jnp.arange(HEADS) == picked, WINDOW, widths).astype(jnp.int32)


def shard_levels(key, shape, split, least, largest):
    factor_of, own = 1.0, jax.random.fold_in(key, 6)
    for dim, parts in split:
        draws = jnp.exp(jax.random.uniform(jax.random.fold_in(own, dim), (parts,), jnp.float32, least / len(split), largest / len(split)))
        factor_of = factor_of * jnp.repeat(draws, shape[dim] // parts).reshape([-1 if axis == dim else 1 for axis in range(len(shape))])
    return factor_of


def length_profile(count, total, most, skew):
    weights = [(1 << 20) // math.isqrt(grade ** skew) + 1 for grade in range(2, count + 1)]
    spare, holding = total - most - (count - 1), [1] * (count - 1)
    while spare > 0:
        free = [i for i in range(count - 1) if holding[i] < most]
        mass, budget = sum([weights[i] for i in free]), spare
        for i in free:
            extra = min(most - holding[i], max(1, budget * weights[i] // mass), spare)
            holding[i] = holding[i] + extra
            spare = spare - extra
    return np.array([most] + holding)


def uneven(stream_key, count, total, bound, lean):
    if count == 2:
        one = jax.random.randint(stream_key, (), max(1, total - bound), min(bound, total - 1) + 1)
        return jnp.stack([one, total - one])
    tallies = jnp.asarray(length_profile(count, total, bound, lean), jnp.int32)
    pairs = (count - 1) // 2
    source_of, taker = tallies[1:1 + 2 * pairs:2], tallies[2:2 + 2 * pairs:2]
    margin = jnp.minimum(source_of - 1, bound - taker)
    passed = jax.random.randint(jax.random.fold_in(stream_key, 1), (pairs,), 0, 1 << 20) % (margin + 1)
    tallies = tallies.at[1:1 + 2 * pairs:2].set(source_of - passed).at[2:2 + 2 * pairs:2].set(taker + passed)
    return tallies[jax.random.permutation(jax.random.fold_in(stream_key, 2), count)]


def normal_values(key, extent, scale, bound, pieces=(), kind=jnp.bfloat16):
    level = shard_levels(key, extent, pieces, -0.22, 0.18) if pieces else 1.0
    entries = jax.random.normal(key, extent, jnp.float32) * scale * level
    return jnp.minimum(jnp.maximum(entries, -bound), bound).astype(kind)


def setup_inputs(seed: int = 0, part: int = 0) -> dict:
    streams_of = jax.random.split(jax.random.key(seed), 14)
    part_keys = jax.random.split(jax.random.fold_in(streams_of[13], part), 14)
    return {
        "prefill_query": draw_prefill_query(jax.random.fold_in(jax.random.fold_in(streams_of[13], part), 71), part),
        "prefill_key": draw_prefill_key(jax.random.fold_in(jax.random.fold_in(streams_of[13], part), 71), part),
        "prefill_value": normal_values(part_keys[2], (TOKENS, KV_HEADS * HD), 1.0, 6.0, ((0, 8), (1, 2))),
        "doc_ids": jnp.searchsorted(jnp.cumsum(uneven(part_keys[3], 4, TOKENS, TOKENS // 2, 1)), jnp.arange(TOKENS), side="right").astype(jnp.int32),
        "head_window": draw_head_window(jax.random.fold_in(streams_of[13], 71), part),
        "dec_query": draw_dec_query(jax.random.fold_in(jax.random.fold_in(streams_of[13], part), 71), part),
        "dec_key": draw_dec_key(jax.random.fold_in(jax.random.fold_in(streams_of[13], part), 71), part),
        "dec_value": normal_values(part_keys[7], (REQS, KV_HEADS * HD), 1.0, 6.0, ((1, 2),)),
        "cache_key": normal_values(part_keys[8], (PAGES * PAGE, KV_HEADS * HD), 1.0, 6.0, ((0, 8), (1, 2))),
        "cache_value": normal_values(part_keys[9], (PAGES * PAGE, KV_HEADS * HD), 1.0, 6.0, ((0, 8), (1, 2))),
        "page_order": jax.random.permutation(part_keys[10], PAGES).astype(jnp.int32),
        "lengths": uneven(part_keys[11], REQS, REQS * MAXLEN // 2, MAXLEN, 2).astype(jnp.int32),
        "out_proj": normal_values(streams_of[12], (HEADS * HD, D), (HEADS * HD) ** -0.5, 0.125, ((0, 2),)),
    }


masked_score = -1e+30

def round_half(values):
    return lax.optimization_barrier(values.astype(jnp.bfloat16)).astype(jnp.float32)

def project(rows_matrix, out_proj):
    columns = HEADS * HD // N_TP
    total = jnp.zeros((rows_matrix.shape[0], D), jnp.float32)
    for group in range(N_TP):
        partial_sum = jnp.dot(rows_matrix[:, group * columns:(group + 1) * columns], out_proj[group * columns:(group + 1) * columns], preferred_element_type=jnp.float32)
        total = total + round_half(partial_sum)
    return total.astype(jnp.bfloat16)

def reference(prefill_query, prefill_key, prefill_value, doc_ids, head_window, dec_query, dec_key, dec_value, cache_key, cache_value, page_order, lengths, out_proj):
    group_size = HEADS // KV_HEADS
    scale_factor = 1.0 / math.sqrt(HD)
    block = math.gcd(512, TOKENS)
    key_pad = jnp.pad(prefill_key, ((WINDOW, 0), (0, 0)))
    value_pad = jnp.pad(prefill_value, ((WINDOW, 0), (0, 0)))
    doc_pad = jnp.pad(doc_ids, (WINDOW, 0), constant_values=-1)
    windows = head_window.reshape(KV_HEADS, group_size)

    def one_block(index):
        start = (index * block).astype(jnp.int32)
        queries = lax.dynamic_slice_in_dim(prefill_query, start, block, 0).reshape(block, KV_HEADS, group_size, HD).astype(jnp.float32)
        keys = lax.dynamic_slice_in_dim(key_pad, start, block + WINDOW, 0).reshape(block + WINDOW, KV_HEADS, HD).astype(jnp.float32)
        values = lax.dynamic_slice_in_dim(value_pad, start, block + WINDOW, 0).reshape(block + WINDOW, KV_HEADS, HD).astype(jnp.float32)
        query_doc = lax.dynamic_slice_in_dim(doc_ids, start, block, 0)
        key_doc = lax.dynamic_slice_in_dim(doc_pad, start, block + WINDOW, 0)
        query_pos = start + jnp.arange(block, dtype=jnp.int32)
        key_pos = start - WINDOW + jnp.arange(block + WINDOW, dtype=jnp.int32)
        gap = query_pos[:, None] - key_pos[None, :]
        allowed = (gap >= 0) & (query_doc[:, None] == key_doc[None, :])
        allowed = allowed[None, None] & (gap[None, None] < windows[:, :, None, None])
        scores = jnp.einsum('tkgd,skd->kgts', queries, keys) * scale_factor
        scores = jnp.where(allowed, scores, masked_score)
        highest = lax.optimization_barrier(jnp.max(scores, axis=-1))
        weights = jnp.where(allowed, jnp.exp(scores - highest[..., None]), 0.0)
        totals = lax.optimization_barrier(jnp.sum(weights, axis=-1))
        output = jnp.einsum('kgts,skd->kgtd', round_half(weights), values) / totals[..., None]
        return output.transpose(2, 0, 1, 3).reshape(block, HEADS * HD).astype(jnp.bfloat16)
    prompt_attn = lax.map(one_block, jnp.arange(TOKENS // block, dtype=jnp.int32)).reshape(TOKENS, HEADS * HD)
    prompt_out = project(prompt_attn, out_proj)
    inverse = jnp.zeros((PAGES,), jnp.int32).at[page_order].set(jnp.arange(PAGES, dtype=jnp.int32))
    cached_keys = cache_key.reshape(PAGES, PAGE, KV_HEADS * HD)[inverse].reshape(REQS, MAXLEN, KV_HEADS, HD).astype(jnp.float32)
    cached_values = cache_value.reshape(PAGES, PAGE, KV_HEADS * HD)[inverse].reshape(REQS, MAXLEN, KV_HEADS, HD).astype(jnp.float32)
    queries = dec_query.reshape(REQS, KV_HEADS, group_size, HD).astype(jnp.float32)
    own_keys = dec_key.reshape(REQS, KV_HEADS, HD).astype(jnp.float32)
    own_values = dec_value.reshape(REQS, KV_HEADS, HD).astype(jnp.float32)
    scores = jnp.einsum('rkgd,rskd->rkgs', queries, cached_keys) * scale_factor
    valid = (jnp.arange(MAXLEN, dtype=jnp.int32)[None, :] < lengths[:, None])[:, None, None, :]
    scores = jnp.where(valid, scores, masked_score)
    own_scores = jnp.einsum('rkgd,rkd->rkg', queries, own_keys) * scale_factor
    highest = jnp.maximum(lax.optimization_barrier(jnp.max(scores, axis=-1)), own_scores)
    weights = jnp.where(valid, jnp.exp(scores - highest[..., None]), 0.0)
    own_weights = jnp.exp(own_scores - highest)
    totals = lax.optimization_barrier(jnp.sum(weights, axis=-1)) + own_weights
    output = jnp.einsum('rkgs,rskd->rkgd', round_half(weights), cached_values) + round_half(own_weights)[..., None] * own_values[:, :, None, :]
    decode_attn = (output / totals[..., None]).reshape(REQS, HEADS * HD).astype(jnp.bfloat16)
    decode_out = project(decode_attn, out_proj)
    return (prompt_out, decode_out)
```

```python
import math

import jax
import jax.numpy as jnp
from jax import lax
from jax.experimental import pallas as pl
from jax.experimental.pallas import tpu as pltpu
from jax.sharding import PartitionSpec as P

HD = 128
PAGE = 128
NEG = -1e30
FLOOR = -8192.0
SCALE2 = math.log2(math.e) / math.sqrt(HD)
LANES = 128


VMEM = pl.BlockSpec(memory_space=pltpu.VMEM)
SMEM = pl.BlockSpec(memory_space=pltpu.SMEM)


def scores_of(q, k):
    return (
        lax.dot_general(q, k, (((1,), (1,)), ((), ())), preferred_element_type=jnp.float32) * SCALE2
    )


def with_ones(v):
    return jnp.concatenate([v, jnp.ones_like(v)], axis=1)


def tiled(column, count):
    return jnp.concatenate([column] * count, axis=1)


def doc_start(info, position):
    start = jnp.int32(0)
    for d in range(1, 4):
        start = jnp.where(position >= info[d], info[d], start)
    return start


def row_docs(info, positions):
    start = jnp.zeros_like(positions)
    for d in range(1, 4):
        start = jnp.where(positions >= info[d], info[d], start)
    return start


def attend_tile(q_ref, keys, values, m_ref, l_ref, acc_ref, rows, group, row_pos, docs, key_pos, win, first, diag, masked):
    heads = q_ref.shape[1] // HD
    repeat = key_pos.shape[1] // LANES
    width = key_pos.shape[1]
    for h in range(heads):
        g = h // group
        columns = slice(h * HD, (h + 1) * HD)
        s = scores_of(q_ref[rows, columns], keys[g])
        if masked:
            low = jnp.maximum(docs, row_pos - win[h] + 1)
            allowed = key_pos >= tiled(low, repeat)
            if diag:
                allowed = allowed & (key_pos <= tiled(row_pos, repeat))
            s = jnp.where(allowed, s, NEG)
        top = jnp.max(s, axis=1, keepdims=True)
        if first:
            fresh = jnp.broadcast_to(top, (s.shape[0], LANES))
        else:
            old = m_ref[h, rows, :]
            fresh = jnp.maximum(old, top)
        p = jnp.exp2(s - tiled(fresh, repeat)).astype(jnp.bfloat16)
        pv = jnp.dot(p, values[g], preferred_element_type=jnp.float32)
        m_ref[h, rows, :] = fresh
        if first:
            l_ref[h, rows, :] = pv[:, HD:]
            acc_ref[rows, columns] = pv[:, :HD]
        else:
            shrink = jnp.exp2(old - fresh)
            l_ref[h, rows, :] = l_ref[h, rows, :] * shrink + pv[:, HD:]
            acc_ref[rows, columns] = acc_ref[rows, columns] * shrink + pv[:, :HD]


def own_kernel(info, win, q_ref, k_ref, v_ref, m_ref, l_ref, acc_ref, *, group, tq):
    rows_all = q_ref.shape[0]
    kv = k_ref.shape[1] // HD
    base = info[0]
    for i in range(rows_all // tq):
        span = (i + 1) * tq
        rows = pl.ds(i * tq, tq)
        row_pos = base + i * tq + lax.broadcasted_iota(jnp.int32, (tq, LANES), 0)
        key_pos = base + lax.broadcasted_iota(jnp.int32, (tq, span), 1)
        keys = [k_ref[:span, g * HD : (g + 1) * HD] for g in range(kv)]
        values = [with_ones(v_ref[:span, g * HD : (g + 1) * HD]) for g in range(kv)]
        attend_tile(
            q_ref, keys, values, m_ref, l_ref, acc_ref, rows, group,
            row_pos, row_docs(info, row_pos), key_pos, win, True, True, True,
        )


def far_kernel(info, win, *refs, group, tq, sources, last):
    refs = list(refs)
    q_ref = refs.pop(0)
    m_in, l_in, acc_in = refs.pop(0), refs.pop(0), refs.pop(0)
    blocks = []
    for distance, count in sources:
        key_refs = [refs.pop(0) for _ in range(count)]
        blocks.append((distance, key_refs, refs.pop(0)))
    if last:
        out_ref = refs.pop(0)
        m_ref, l_ref, acc_ref = refs
    else:
        m_ref, l_ref, acc_ref = refs
    rows_all = q_ref.shape[0]
    kv = blocks[0][2].shape[1] // HD
    heads = q_ref.shape[1] // HD
    base = info[0]
    odd = info[4]
    half = info[5]
    least, most = win[0], win[0]
    for h in range(1, heads):
        least, most = jnp.minimum(least, win[h]), jnp.maximum(most, win[h])
    m_ref[...] = m_in[...]
    l_ref[...] = l_in[...]
    acc_ref[...] = acc_in[...]

    def q_tile(i, _):
        first_row = base + i * tq
        last_row = first_row + tq - 1
        rows = pl.ds(pl.multiple_of(i * tq, tq), tq)
        need_low = jnp.maximum(doc_start(info, first_row), first_row - most + 1)
        full_low = jnp.maximum(doc_start(info, last_row), last_row - least + 1)
        for distance, key_refs, v_ref in blocks:
            span = v_ref.shape[0]
            key_base = base - distance * span
            needed = (key_base >= 0) & (key_base + span - 1 >= need_low)
            full = key_base >= full_low

            def body(masked, key_base=key_base, key_refs=key_refs, v_ref=v_ref, span=span):
                keys = []
                for g in range(kv):
                    part = slice(g * HD, (g + 1) * HD)
                    if len(key_refs) == 1:
                        keys.append(key_refs[0][:, part])
                    else:
                        keys.append(jnp.where(odd == 1, key_refs[0][:, part], key_refs[1][:, part]))
                values = [with_ones(v_ref[:, g * HD : (g + 1) * HD]) for g in range(kv)]
                row_pos = first_row + lax.broadcasted_iota(jnp.int32, (tq, LANES), 0)
                key_pos = key_base + lax.broadcasted_iota(jnp.int32, (tq, span), 1)
                docs = row_docs(info, row_pos) if masked else None
                attend_tile(
                    q_ref, keys, values, m_ref, l_ref, acc_ref, rows, group,
                    row_pos, docs, key_pos, win, False, False, masked,
                )

            pl.when(needed & full)(lambda body=body: body(False))
            pl.when(needed & jnp.logical_not(full))(lambda body=body: body(True))
        return 0

    lax.fori_loop(0, rows_all // tq, q_tile, 0)
    if last:
        per = rows_all // 2
        for part in range(2):
            where_to = jnp.where(half == part, per, 0)
            source = pl.ds(part * per, per)
            for h in range(heads):
                columns = slice(h * HD, (h + 1) * HD)
                value = acc_ref[source, columns] / l_ref[h, source, :]
                out_ref[pl.ds(pl.multiple_of(where_to, per), per), columns] = value.astype(jnp.bfloat16)


def decode_kernel(owner, limit, flag, q_ref, ok_ref, ov_ref, k_ref, v_ref, acc_out, stat_out, s_ref, *, group):
    requests = ok_ref.shape[0]
    rows = group * requests
    pages = k_ref.shape[0] // PAGE
    g = pl.program_id(0)
    q = jnp.concatenate([q_ref[:, j * HD : (j + 1) * HD] for j in range(group)], axis=0)
    request = lax.broadcasted_iota(jnp.int32, (requests, LANES), 0)
    request = jnp.concatenate([request] * group, axis=0)
    lane = lax.broadcasted_iota(jnp.int32, (rows, LANES), 1)
    own = scores_of(q, ok_ref[...])
    own_lane = lax.broadcasted_iota(jnp.int32, (rows, requests), 1)
    own_row = jnp.concatenate([lax.broadcasted_iota(jnp.int32, (requests, requests), 0)] * group, axis=0)
    own = jnp.where((own_row == own_lane) & (flag[0] == 0), own, NEG)
    top = jnp.full((rows, LANES), NEG, jnp.float32)
    for p in range(pages):
        s = scores_of(q, k_ref[p * PAGE : (p + 1) * PAGE, :])
        edge = jnp.where(request == owner[p], limit[p], 0)
        s = jnp.where(lane < edge, s, NEG)
        s_ref[:, p * PAGE : (p + 1) * PAGE] = s
        top = jnp.maximum(top, s)
    top = jnp.maximum(jnp.max(top, axis=1, keepdims=True), jnp.max(own, axis=1, keepdims=True))
    top = jnp.maximum(jnp.ceil(top * (1.0 / 32.0)) * 32.0, FLOOR)
    top = jnp.broadcast_to(top, (rows, LANES))
    weights = jnp.exp2(s_ref[...] - tiled(top, pages)).astype(jnp.bfloat16)
    pv = jnp.dot(weights, with_ones(v_ref[...]), preferred_element_type=jnp.float32)
    own_weights = jnp.exp2(own - top[:, :requests]).astype(jnp.bfloat16)
    pv = pv + jnp.dot(own_weights, with_ones(ov_ref[...]), preferred_element_type=jnp.float32)
    stats = jnp.zeros((requests, LANES), jnp.float32)
    spot = lax.broadcasted_iota(jnp.int32, (requests, LANES), 1)
    for j in range(group):
        part = slice(j * requests, (j + 1) * requests)
        acc_out[:, j * HD : (j + 1) * HD] = pv[part, :HD].astype(jnp.bfloat16)
        total = pv[part, HD:]
        high = total.astype(jnp.bfloat16).astype(jnp.float32)
        stats = jnp.where(spot == j, top[part], stats)
        stats = jnp.where(spot == group + j, high, stats)
        stats = jnp.where(spot == 2 * group + j, total - high, stats)
    stat_out[...] = stats.astype(jnp.bfloat16)


def merge_kernel(info, a_ref, b_ref, out_ref, *, group, last):
    requests, width = a_ref.shape
    kv = width // (group * HD + LANES)
    body = kv * group * HD
    spot = lax.broadcasted_iota(jnp.int32, (requests, LANES), 1)
    for g in range(kv):
        tile = slice(body + g * LANES, body + (g + 1) * LANES)
        left, right = a_ref[:, tile].astype(jnp.float32), b_ref[:, tile].astype(jnp.float32)
        stats = jnp.zeros((requests, LANES), jnp.float32)
        for j in range(group):
            columns = slice((g * group + j) * HD, (g * group + j + 1) * HD)
            m1, m2 = left[:, j : j + 1], right[:, j : j + 1]
            l1 = left[:, group + j : group + j + 1] + left[:, 2 * group + j : 2 * group + j + 1]
            l2 = right[:, group + j : group + j + 1] + right[:, 2 * group + j : 2 * group + j + 1]
            top = jnp.maximum(m1, m2)
            e1, e2 = jnp.exp2(m1 - top), jnp.exp2(m2 - top)
            total = l1 * e1 + l2 * e2
            value = a_ref[:, columns].astype(jnp.float32) * e1 + b_ref[:, columns].astype(jnp.float32) * e2
            if last:
                value = (value / total).astype(jnp.bfloat16)
                per = requests // 2
                half = info[5]
                for part in range(2):
                    where_to = jnp.where(half == part, per, 0)
                    out_ref[pl.ds(pl.multiple_of(where_to, per), per), columns] = value[part * per : (part + 1) * per]
            else:
                out_ref[:, columns] = value.astype(jnp.bfloat16)
                high = total.astype(jnp.bfloat16).astype(jnp.float32)
                stats = jnp.where(spot == j, top, stats)
                stats = jnp.where(spot == group + j, high, stats)
                stats = jnp.where(spot == 2 * group + j, total - high, stats)
        if not last:
            out_ref[:, tile] = stats.astype(jnp.bfloat16)


def project_kernel(a_ref, d_ref, w_ref, out_ref):
    w = w_ref[...]
    split = a_ref.shape[0]
    out_ref[:split, :] = jnp.dot(a_ref[...], w, preferred_element_type=jnp.float32).astype(jnp.bfloat16)
    out_ref[split:, :] = jnp.dot(d_ref[...], w, preferred_element_type=jnp.float32).astype(jnp.bfloat16)


def finish_kernel(a_ref, d_ref, w_ref, r_ref, *rest):
    po_ref, do_ref = rest[-2:]
    w = w_ref[...]
    split = a_ref.shape[0]

    def total(x, received):
        mine = jnp.dot(x, w, preferred_element_type=jnp.float32).astype(jnp.bfloat16)
        return (mine.astype(jnp.float32) + received.astype(jnp.float32)).astype(jnp.bfloat16)

    po_ref[...] = total(a_ref[...], r_ref[:split, :])
    do_ref[...] = total(d_ref[...], r_ref[split:, :])


def on_device(
    prefill_query, prefill_key, prefill_value, doc_ids, head_window,
    dec_query, dec_key, dec_value, cache_key, cache_value, page_order, lengths, out_proj,
):
    n = lax.axis_size("seq")
    tokens, width = prefill_query.shape
    kv = prefill_key.shape[1] // HD
    heads = width // HD
    group = heads // kv
    reach = n // 2
    tq = math.gcd(tokens, 256)
    s = lax.axis_index("seq")
    half = lax.axis_index("tp")
    odd = s % 2
    f32, bf16, i32 = jnp.float32, jnp.bfloat16, jnp.int32

    def ring(x, by):
        return lax.ppermute(x, "seq", [(i, (i + by) % n) for i in range(n)])

    def swap(x, bit=1):
        return lax.ppermute(x, "seq", [(i, i ^ bit) for i in range(n)])

    def pick(even_value, odd_value):
        return jnp.where(odd == 1, odd_value, even_value)

    starts = jnp.sum(doc_ids[None, :] < jnp.arange(1, 4, dtype=i32)[:, None], axis=1, dtype=i32)
    info = jnp.concatenate([jnp.stack([(s * tokens).astype(i32)]), starts, jnp.stack([odd.astype(i32), half.astype(i32)])])

    v_even = {0: prefill_value}
    k_even = {0: prefill_key}
    k_swapped = [swap(prefill_key)]
    back = prefill_value
    for d in range(2, reach + 1, 2):
        if d < reach:
            v_even[d] = ring(v_even[d - 2], 2)
        k_even[d] = ring(k_even[d - 2], 2)
        back = ring(back, -2)
        k_swapped.append(ring(k_swapped[-1], 2)) if d < reach else None
    v_even[reach] = back
    k_last = swap(k_even[reach])
    keys, values = {}, {}
    for d in range(2, reach + 1, 2):
        keys[d], values[d] = [k_even[d]], v_even[d]
    for d in range(1, reach, 2):
        keys[d] = [k_swapped[d // 2], k_swapped[d // 2 + 1] if d + 1 < reach else k_last]
        values[d] = swap(pick(v_even[d - 1], v_even[d + 1]))

    state = [
        jax.ShapeDtypeStruct((heads, tokens, LANES), f32),
        jax.ShapeDtypeStruct((heads, tokens, LANES), f32),
        jax.ShapeDtypeStruct((tokens, width), f32),
    ]

    pages = page_order.shape[0]
    requests = dec_query.shape[0]
    per_request = pages * n // requests
    owner = page_order // per_request
    limit = jnp.clip(lengths[owner] - (page_order % per_request) * PAGE, 0, PAGE)
    wide = group * HD
    acc, stat = pl.pallas_call(
        lambda *refs: decode_kernel(*refs, group=group),
        grid=(kv,),
        in_specs=[
            SMEM, SMEM, SMEM,
            pl.BlockSpec((requests, wide), lambda g: (0, g)),
            pl.BlockSpec((requests, HD), lambda g: (0, g)),
            pl.BlockSpec((requests, HD), lambda g: (0, g)),
            pl.BlockSpec((pages * PAGE, HD), lambda g: (0, g)),
            pl.BlockSpec((pages * PAGE, HD), lambda g: (0, g)),
        ],
        out_specs=[
            pl.BlockSpec((requests, wide), lambda g: (0, g)),
            pl.BlockSpec((requests, LANES), lambda g: (0, g)),
        ],
        out_shape=[
            jax.ShapeDtypeStruct((requests, kv * wide), bf16),
            jax.ShapeDtypeStruct((requests, kv * LANES), bf16),
        ],
        scratch_shapes=[pltpu.VMEM((group * requests, pages * PAGE), f32)],
        cost_estimate=pl.CostEstimate(flops=4 * 10**9, transcendentals=0, bytes_accessed=4 << 20),
        name="decode_pages",
    )(owner, limit, jnp.stack([s.astype(i32)]), dec_query, dec_key, dec_value, cache_key, cache_value)
    partial = jnp.concatenate([acc, stat], axis=1)
    bit = 1
    while bit < n:
        last = bit * 2 >= n
        other = swap(partial, bit)
        partial = pl.pallas_call(
            lambda *refs, last=last: merge_kernel(*refs, group=group, last=last),
            in_specs=[SMEM, VMEM, VMEM],
            out_specs=VMEM,
            out_shape=jax.ShapeDtypeStruct((requests, kv * wide if last else partial.shape[1]), bf16),
            cost_estimate=pl.CostEstimate(flops=10**9, transcendentals=0, bytes_accessed=1 << 18),
            name="decode_merge",
        )(info, partial, other)
        bit *= 2
    decode_attn = partial

    carry = pl.pallas_call(
        lambda *refs: own_kernel(*refs, group=group, tq=tq),
        in_specs=[SMEM, SMEM] + [VMEM] * 3,
        out_specs=[VMEM] * 3,
        out_shape=state,
        cost_estimate=pl.CostEstimate(flops=3 * 10**9, transcendentals=0, bytes_accessed=4 << 20),
        name="prompt_own",
    )(info, head_window, prefill_query, prefill_key, prefill_value)
    order = [d for d in (2, 1, 4, 3) if d <= reach] + list(range(5, reach + 1))
    stages = [order[i : i + 2] for i in range(0, len(order), 2)]
    for index, stage in enumerate(stages):
        last = index == len(stages) - 1
        sources = [(d, len(keys[d])) for d in stage]
        operands = [x for d in stage for x in (*keys[d], values[d])]
        scratch = [pltpu.VMEM(x.shape, x.dtype) for x in state] if last else []
        carry = pl.pallas_call(
            lambda *refs, sources=sources, last=last: far_kernel(
                *refs, group=group, tq=tq, sources=sources, last=last
            ),
            in_specs=[SMEM, SMEM] + [VMEM] * (4 + len(operands)),
            out_specs=VMEM if last else [VMEM] * 3,
            out_shape=jax.ShapeDtypeStruct((tokens, width), bf16) if last else state,
            scratch_shapes=scratch,
            cost_estimate=pl.CostEstimate(flops=5 * 10**9, transcendentals=0, bytes_accessed=8 << 20),
            name="prompt_far",
        )(info, head_window, prefill_query, *carry, *operands)
    attn = carry

    model = out_proj.shape[1]
    chunks = 4
    cols = model // chunks
    tr, dr = tokens // 2, requests // 2
    theirs_specs = [
        pl.BlockSpec((tr, width), lambda j: (0, 0)),
        pl.BlockSpec((dr, width), lambda j: (0, 0)),
    ]
    ours_specs = [
        pl.BlockSpec((tr, width), lambda j: (1, 0)),
        pl.BlockSpec((dr, width), lambda j: (1, 0)),
    ]
    tn = math.gcd(cols, 512)
    steps = cols // tn
    received = []
    for c in range(chunks):
        sent = pl.pallas_call(
            project_kernel,
            grid=(steps,),
            in_specs=theirs_specs + [pl.BlockSpec((width, tn), lambda j, c=c: (0, c * steps + j))],
            out_specs=pl.BlockSpec((tr + dr, tn), lambda j: (0, j)),
            out_shape=jax.ShapeDtypeStruct((tr + dr, cols), bf16),
            cost_estimate=pl.CostEstimate(flops=10**9, transcendentals=0, bytes_accessed=3 << 20),
            name="project_theirs",
        )(attn, decode_attn, out_proj)
        received.append(lax.ppermute(sent, "tp", [(0, 1), (1, 0)]))
    outs = ()
    for c in range(chunks):
        outs = pl.pallas_call(
            finish_kernel,
            grid=(steps,),
            in_specs=ours_specs
            + [
                pl.BlockSpec((width, tn), lambda j, c=c: (0, c * steps + j)),
                pl.BlockSpec((tr + dr, tn), lambda j: (0, j)),
            ]
            + [pl.BlockSpec(memory_space=pl.ANY)] * len(outs),
            out_specs=[
                pl.BlockSpec((tr, tn), lambda j, c=c: (0, c * steps + j)),
                pl.BlockSpec((dr, tn), lambda j, c=c: (0, c * steps + j)),
            ],
            out_shape=[jax.ShapeDtypeStruct((tr, model), bf16), jax.ShapeDtypeStruct((dr, model), bf16)],
            input_output_aliases={4: 0, 5: 1} if outs else {},
            cost_estimate=pl.CostEstimate(flops=10**9, transcendentals=0, bytes_accessed=4 << 20),
            name="project_ours",
        )(attn, decode_attn, out_proj, received[c], *outs)
    return tuple(outs)


def solution(mesh):
    placed = (
        P(("rep", "seq"), "tp"),
        P(("rep", "seq"), "tp"),
        P(("rep", "seq"), "tp"),
        P("rep"),
        P("tp"),
        P("rep", "tp"),
        P("rep", "tp"),
        P("rep", "tp"),
        P(("rep", "seq"), "tp"),
        P(("rep", "seq"), "tp"),
        P(("rep", "seq")),
        P("rep"),
        P("tp", None),
    )
    return jax.shard_map(
        on_device,
        mesh=mesh,
        in_specs=placed,
        out_specs=(P(("rep", "seq", "tp"), None), P(("rep", "tp"), None)),
        check_vma=False,
    )
```

```python
import math

import jax
import jax.numpy as jnp
from jax import lax
from jax.experimental import pallas as pl
from jax.experimental.pallas import tpu as pltpu
from jax.sharding import PartitionSpec as P

HD = 128
PAGE = 128
NEG = -1e30
FLOOR = -8192.0
SCALE2 = math.log2(math.e) / math.sqrt(HD)
LANES = 128
EXTRA = 16
DOCS = 4
COST = 10**8


VMEM = pl.BlockSpec(memory_space=pltpu.VMEM)
SMEM = pl.BlockSpec(memory_space=pltpu.SMEM)


def scores_of(k, q):
    return (
        lax.dot_general(k, q, (((1,), (1,)), ((), ())), preferred_element_type=jnp.float32) * SCALE2
    )


def flipped(v):
    return jnp.concatenate([v.T, jnp.ones((EXTRA, v.shape[0]), v.dtype)], axis=0)


def doc_starts(doc_ref):
    ids = doc_ref[...]
    return [jnp.sum((ids < d).astype(jnp.int32)) for d in range(1, DOCS)]


def start_at(starts, position):
    start = jnp.zeros_like(position)
    for edge in starts:
        start = jnp.where(position >= edge, edge, start)
    return start


def attend_tile(q, keys, values, state, i, row_pos, docs, key_pos, win, first, diag, masked):
    m_ref, l_ref, acc_ref = state
    heads = m_ref.shape[1]
    group = heads // len(keys)
    for h in range(heads):
        g = h // group
        columns = slice(h * HD, (h + 1) * HD)
        s = scores_of(keys[g], q(columns))
        if masked:
            allowed = key_pos >= jnp.maximum(docs, row_pos - win[h] + 1)
            if diag:
                allowed = allowed & (key_pos <= row_pos)
            s = jnp.where(allowed, s, NEG)
        top = jnp.max(s, axis=0, keepdims=True)
        if first:
            fresh = top
        else:
            old = m_ref[i, h : h + 1, :]
            fresh = jnp.maximum(old, top)
        p = jnp.exp2(s - fresh).astype(jnp.bfloat16)
        pv = jnp.dot(values[g], p, preferred_element_type=jnp.float32)
        m_ref[i, h : h + 1, :] = fresh
        if first:
            l_ref[i, h : h + 1, :] = pv[HD : HD + 1, :]
            acc_ref[i, columns, :] = pv[:HD, :]
        else:
            shrink = jnp.exp2(old - fresh)
            l_ref[i, h : h + 1, :] = l_ref[i, h : h + 1, :] * shrink + pv[HD : HD + 1, :]
            acc_ref[i, columns, :] = acc_ref[i, columns, :] * shrink + pv[:HD, :]


def own_kernel(win, doc_ref, q_ref, k_ref, v_ref, info_ref, m_ref, l_ref, acc_ref):
    tiles, _, tq = m_ref.shape
    kv = k_ref.shape[1] // HD
    base = lax.axis_index("seq") * (tiles * tq)
    starts = doc_starts(doc_ref)
    for d, start in enumerate(starts):
        info_ref[d] = start
    whole = [flipped(v_ref[:, g * HD : (g + 1) * HD]) for g in range(kv)]
    for i in range(tiles):
        span = (i + 1) * tq
        row_pos = base + i * tq + lax.broadcasted_iota(jnp.int32, (1, tq), 1)
        key_pos = base + lax.broadcasted_iota(jnp.int32, (span, tq), 0)
        keys = [k_ref[:span, g * HD : (g + 1) * HD] for g in range(kv)]
        values = [v[:, :span] for v in whole]
        attend_tile(
            lambda columns, i=i: q_ref[i * tq : (i + 1) * tq, columns],
            keys, values, (m_ref, l_ref, acc_ref), i,
            row_pos, start_at(starts, row_pos), key_pos, win, True, True, True,
        )


def far_kernel(win, info, *refs, sources, last):
    refs = list(refs)
    q_ref, m_in, l_in, acc_in = refs[:4]
    refs = refs[4:]
    blocks = []
    for distance, count in sources:
        blocks.append((distance, refs[:count], refs[count]))
        refs = refs[count + 1 :]
    if last:
        out_ref = refs.pop(0)
    m_ref, l_ref, acc_ref, v_scratch = refs
    tiles, heads, tq = m_ref.shape
    kv = blocks[0][2].shape[1] // HD
    seq = lax.axis_index("seq")
    base = seq * (tiles * tq)
    odd = seq % 2
    starts = [info[d] for d in range(DOCS - 1)]
    least, most = win[0], win[0]
    for h in range(1, heads):
        least, most = jnp.minimum(least, win[h]), jnp.maximum(most, win[h])
    m_ref[...] = m_in[...]
    l_ref[...] = l_in[...]
    acc_ref[...] = acc_in[...]
    for index, (_, _, v_ref) in enumerate(blocks):
        for g in range(kv):
            v_scratch[index, g] = flipped(v_ref[:, g * HD : (g + 1) * HD])

    def q_tile(i, _):
        first_row = base + i * tq
        last_row = first_row + tq - 1
        need_low = jnp.maximum(start_at(starts, first_row), first_row - most + 1)
        full_low = jnp.maximum(start_at(starts, last_row), last_row - least + 1)
        for index, (distance, key_refs, v_ref) in enumerate(blocks):
            span = v_ref.shape[0]
            key_base = base - distance * span
            needed = (key_base >= 0) & (key_base + span - 1 >= need_low)
            full = key_base >= full_low

            def body(masked, index=index, key_base=key_base, key_refs=key_refs, span=span):
                keys = []
                for g in range(kv):
                    part = slice(g * HD, (g + 1) * HD)
                    if len(key_refs) == 1:
                        keys.append(key_refs[0][:, part])
                    else:
                        keys.append(jnp.where(odd == 1, key_refs[0][:, part], key_refs[1][:, part]))
                values = [v_scratch[index, g] for g in range(kv)]
                row_pos = first_row + lax.broadcasted_iota(jnp.int32, (1, tq), 1)
                key_pos = key_base + lax.broadcasted_iota(jnp.int32, (span, tq), 0)
                attend_tile(
                    lambda columns: q_ref[pl.ds(pl.multiple_of(i * tq, tq), tq), columns],
                    keys, values, (m_ref, l_ref, acc_ref), i,
                    row_pos, start_at(starts, row_pos) if masked else None, key_pos, win, False, False, masked,
                )

            pl.when(needed & full)(lambda body=body: body(False))
            pl.when(needed & jnp.logical_not(full))(lambda body=body: body(True))
        return 0

    lax.fori_loop(0, tiles, q_tile, 0)
    if last:
        half = lax.axis_index("tp")
        for i in range(tiles):
            place = pl.ds(pl.multiple_of(jnp.where(half == i, tq, 0), tq), tq)
            for h in range(heads):
                columns = slice(h * HD, (h + 1) * HD)
                value = acc_ref[i, columns, :] / l_ref[i, h : h + 1, :]
                out_ref[place, columns] = value.T.astype(jnp.bfloat16)


def decode_kernel(order, lengths, q_ref, ok_ref, ov_ref, k_ref, v_ref, out_ref, s_ref, *, per_request):
    requests = ok_ref.shape[0]
    group = q_ref.shape[1] // HD
    lanes = group * requests
    pages = k_ref.shape[0] // PAGE
    q = jnp.concatenate([q_ref[:, j * HD : (j + 1) * HD] for j in range(group)], axis=0)
    request = jnp.concatenate([lax.broadcasted_iota(jnp.int32, (1, requests), 1)] * group, axis=1)
    place = lax.broadcasted_iota(jnp.int32, (PAGE, lanes), 0)
    own = scores_of(ok_ref[...], q)
    own_row = lax.broadcasted_iota(jnp.int32, (requests, lanes), 0)
    own = jnp.where((own_row == request) & (lax.axis_index("seq") == 0), own, NEG)
    tops = jnp.max(own.reshape(requests // 8, 8, lanes), axis=0)
    for p in range(pages):
        s = scores_of(k_ref[p * PAGE : (p + 1) * PAGE, :], q)
        code = order[p]
        owner = code // per_request
        limit = lengths[owner] - (code - owner * per_request) * PAGE
        s = jnp.where(place < jnp.where(request == owner, limit, 0), s, NEG)
        s_ref[p * PAGE : (p + 1) * PAGE, :] = s
        tops = jnp.maximum(tops, jnp.max(s.reshape(PAGE // 8, 8, lanes), axis=0))
    top = jnp.max(tops, axis=0, keepdims=True)
    top = jnp.maximum(jnp.ceil(top * (1.0 / 32.0)) * 32.0, FLOOR)
    weights = jnp.exp2(s_ref[...] - top).astype(jnp.bfloat16)
    pv = jnp.dot(flipped(v_ref[...]), weights, preferred_element_type=jnp.float32)
    own_weights = jnp.exp2(own - top).astype(jnp.bfloat16)
    pv = pv + jnp.dot(flipped(ov_ref[...]), own_weights, preferred_element_type=jnp.float32)
    out_ref[:HD, :] = pv[:HD, :].astype(jnp.bfloat16)
    out_ref[HD:, :] = packed_stats(top, pv[HD : HD + 1, :])


def packed_stats(top, total):
    high = total.astype(jnp.bfloat16).astype(jnp.float32)
    row = lax.broadcasted_iota(jnp.int32, (EXTRA, top.shape[1]), 0)
    stats = jnp.where(row == 0, top, jnp.where(row == 1, high, total - high))
    return stats.astype(jnp.bfloat16)


def merge_kernel(a_ref, b_ref, out_ref, *, requests, last):
    rows, lanes = a_ref.shape
    kv = rows // (HD + EXTRA)
    group = lanes // requests
    f32 = jnp.float32
    for g in range(kv):
        base = g * (HD + EXTRA)
        body, tile = slice(base, base + HD), slice(base + HD, base + HD + EXTRA)
        left, right = a_ref[tile, :].astype(f32), b_ref[tile, :].astype(f32)
        top = jnp.maximum(left[0:1], right[0:1])
        e1, e2 = jnp.exp2(left[0:1] - top), jnp.exp2(right[0:1] - top)
        total = (left[1:2] + left[2:3]) * e1 + (right[1:2] + right[2:3]) * e2
        value = a_ref[body, :].astype(f32) * e1 + b_ref[body, :].astype(f32) * e2
        if not last:
            out_ref[body, :] = value.astype(jnp.bfloat16)
            out_ref[tile, :] = packed_stats(top, total)
            continue
        value = (value / total).T.astype(jnp.bfloat16)
        per = requests // 2
        half = lax.axis_index("tp")
        for j in range(group):
            columns = slice((g * group + j) * HD, (g * group + j + 1) * HD)
            for part in range(2):
                place = pl.ds(pl.multiple_of(jnp.where(half == part, per, 0), per), per)
                start = j * requests + part * per
                out_ref[place, columns] = value[start : start + per, :]


def product(x, w):
    return jnp.dot(x, w, preferred_element_type=jnp.float32).astype(jnp.bfloat16)


def project_kernel(a_ref, d_ref, w_ref, out_ref, *, column, second):
    tr, dr = a_ref.shape[0] // 2, d_ref.shape[0] // 2
    a = a_ref[second * tr : (second + 1) * tr, :]
    d = d_ref[second * dr : (second + 1) * dr, :]
    step = math.gcd(out_ref.shape[1], 512)
    for c in range(0, out_ref.shape[1], step):
        w = w_ref[:, column + c : column + c + step]
        out_ref[:tr, c : c + step] = product(a, w)
        out_ref[tr:, c : c + step] = product(d, w)


def finish_kernel(a_ref, d_ref, w_ref, mine_ref, r0_ref, r1_ref, po_ref, do_ref):
    tr, dr = po_ref.shape[0], do_ref.shape[0]
    tn = po_ref.shape[1]
    j = pl.program_id(0)
    early = mine_ref.shape[1] // tn

    def add(x, y):
        return (x.astype(jnp.float32) + y.astype(jnp.float32)).astype(jnp.bfloat16)

    @pl.when(j < early)
    def _():
        here = pl.ds(pl.multiple_of(j * tn, tn), tn)
        po_ref[...] = add(mine_ref[:tr, here], r0_ref[:tr, here])
        do_ref[...] = add(mine_ref[tr:, here], r0_ref[tr:, here])

    @pl.when(j >= early)
    def _():
        here = pl.ds(pl.multiple_of((j - early) * tn, tn), tn)
        w = w_ref[:, pl.ds(pl.multiple_of(j * tn, tn), tn)]
        po_ref[...] = add(product(a_ref[tr:, :], w), r1_ref[:tr, here])
        do_ref[...] = add(product(d_ref[dr:, :], w), r1_ref[tr:, here])


def on_device(
    prefill_query, prefill_key, prefill_value, doc_ids, head_window,
    dec_query, dec_key, dec_value, cache_key, cache_value, page_order, lengths, out_proj,
):
    n = lax.axis_size("seq")
    tokens, width = prefill_query.shape
    kv = prefill_key.shape[1] // HD
    heads = width // HD
    reach = n // 2
    tiles, tq = 2, tokens // 2
    odd = lax.axis_index("seq") % 2
    f32, bf16, i32 = jnp.float32, jnp.bfloat16, jnp.int32

    def ring(x, by):
        return lax.ppermute(x, "seq", [(i, (i + by) % n) for i in range(n)])

    def swap(x, bit=1):
        return lax.ppermute(x, "seq", [(i, i ^ bit) for i in range(n)])

    def pick(even_value, odd_value):
        return jnp.where(odd == 1, odd_value, even_value)

    def params(mib):
        return pltpu.CompilerParams(vmem_limit_bytes=mib << 20)

    def cost(us):
        return pl.CostEstimate(flops=int(us * COST), transcendentals=0, bytes_accessed=1 << 20)

    v_even = {0: prefill_value}
    k_even = {0: prefill_key}
    k_swapped = [swap(prefill_key)]
    back = prefill_value
    for d in range(2, reach + 1, 2):
        if d < reach:
            v_even[d] = ring(v_even[d - 2], 2)
            k_swapped.append(ring(k_swapped[-1], 2))
        k_even[d] = ring(k_even[d - 2], 2)
        back = ring(back, -2)
    v_even[reach] = back
    k_last = swap(k_even[reach])
    keys, values = {}, {}
    for d in range(2, reach + 1, 2):
        keys[d], values[d] = [k_even[d]], v_even[d]
    for d in range(1, reach, 2):
        keys[d] = [k_swapped[d // 2], k_swapped[d // 2 + 1] if d + 1 < reach else k_last]
        values[d] = swap(pick(v_even[d - 1], v_even[d + 1]))

    pages = page_order.shape[0]
    requests = dec_query.shape[0]
    group = heads // kv
    tall = HD + EXTRA
    partial = pl.pallas_call(
        lambda *refs: decode_kernel(*refs, per_request=pages * n // requests),
        grid=(kv,),
        in_specs=[
            SMEM, SMEM,
            pl.BlockSpec((requests, group * HD), lambda g: (0, g)),
            pl.BlockSpec((requests, HD), lambda g: (0, g)),
            pl.BlockSpec((requests, HD), lambda g: (0, g)),
            pl.BlockSpec((pages * PAGE, HD), lambda g: (0, g)),
            pl.BlockSpec((pages * PAGE, HD), lambda g: (0, g)),
        ],
        out_specs=pl.BlockSpec((tall, group * requests), lambda g: (g, 0)),
        out_shape=jax.ShapeDtypeStruct((kv * tall, group * requests), bf16),
        scratch_shapes=[pltpu.VMEM((pages * PAGE, group * requests), f32)],
        cost_estimate=cost(5),
        compiler_params=params(24),
        name="decode_pages",
    )(page_order, lengths, dec_query, dec_key, dec_value, cache_key, cache_value)
    bit = 1
    while bit < n:
        last = bit * 2 >= n
        other = swap(partial, bit)
        partial = pl.pallas_call(
            lambda *refs, last=last: merge_kernel(*refs, requests=requests, last=last),
            in_specs=[VMEM, VMEM],
            out_specs=VMEM,
            out_shape=jax.ShapeDtypeStruct((requests, width) if last else partial.shape, bf16),
            cost_estimate=cost(1),
            compiler_params=params(4),
            name="decode_merge",
        )(partial, other)
        bit *= 2
    decode_attn = partial

    state = [
        jax.ShapeDtypeStruct((tiles, heads, tq), f32),
        jax.ShapeDtypeStruct((tiles, heads, tq), f32),
        jax.ShapeDtypeStruct((tiles, width, tq), f32),
    ]
    info, *carry = pl.pallas_call(
        own_kernel,
        in_specs=[SMEM] + [VMEM] * 4,
        out_specs=[SMEM] + [VMEM] * 3,
        out_shape=[jax.ShapeDtypeStruct((DOCS - 1,), i32)] + state,
        cost_estimate=cost(3),
        compiler_params=params(12),
        name="prompt_own",
    )(head_window, doc_ids.reshape(-1, LANES), prefill_query, prefill_key, prefill_value)
    order = [d for d in (2, 1, 4, 3) if d <= reach] + list(range(5, reach + 1))
    stages = [order[i : i + 2] for i in range(0, len(order), 2)]
    for index, stage in enumerate(stages):
        last = index == len(stages) - 1
        sources = [(d, len(keys[d])) for d in stage]
        operands = [x for d in stage for x in (*keys[d], values[d])]
        scratch = [pltpu.VMEM(x.shape, x.dtype) for x in state] if last else []
        scratch.append(pltpu.VMEM((len(stage), kv, tall, tokens), bf16))
        carry = pl.pallas_call(
            lambda *refs, sources=sources, last=last: far_kernel(*refs, sources=sources, last=last),
            in_specs=[SMEM, SMEM] + [VMEM] * (4 + len(operands)),
            out_specs=VMEM if last else [VMEM] * 3,
            out_shape=jax.ShapeDtypeStruct((tokens, width), bf16) if last else state,
            scratch_shapes=scratch,
            cost_estimate=cost(5),
            compiler_params=params(16),
            name="prompt_far",
        )(head_window, info, prefill_query, *carry, *operands)
    attn = carry

    model = out_proj.shape[1]
    tr, dr = tokens // 2, requests // 2
    cols = model // 2

    def project(column, second):
        return pl.pallas_call(
            lambda *refs: project_kernel(*refs, column=column, second=second),
            in_specs=[VMEM] * 3,
            out_specs=VMEM,
            out_shape=jax.ShapeDtypeStruct((tr + dr, cols), bf16),
            cost_estimate=cost(2),
            compiler_params=params(16),
            name="project_own" if second else "project_theirs",
        )(attn, decode_attn, out_proj)

    received = [lax.ppermute(project(c * cols, 0), "tp", [(0, 1), (1, 0)]) for c in range(2)]
    mine = project(0, 1)
    tn = math.gcd(cols, 512)
    return tuple(
        pl.pallas_call(
            finish_kernel,
            grid=(model // tn,),
            in_specs=[VMEM] * 6,
            out_specs=[
                pl.BlockSpec((tr, tn), lambda j: (0, j)),
                pl.BlockSpec((dr, tn), lambda j: (0, j)),
            ],
            out_shape=[jax.ShapeDtypeStruct((tr, model), bf16), jax.ShapeDtypeStruct((dr, model), bf16)],
            cost_estimate=cost(3),
            compiler_params=params(20),
            name="project_finish",
        )(attn, decode_attn, out_proj, mine, *received)
    )


def solution(mesh):
    placed = (
        P(("rep", "seq"), "tp"),
        P(("rep", "seq"), "tp"),
        P(("rep", "seq"), "tp"),
        P("rep"),
        P("tp"),
        P("rep", "tp"),
        P("rep", "tp"),
        P("rep", "tp"),
        P(("rep", "seq"), "tp"),
        P(("rep", "seq"), "tp"),
        P(("rep", "seq")),
        P("rep"),
        P("tp", None),
    )
    return jax.shard_map(
        on_device,
        mesh=mesh,
        in_specs=placed,
        out_specs=(P(("rep", "seq", "tp"), None), P(("rep", "tp"), None)),
        check_vma=False,
    )
```

```python
import math

import jax
import jax.numpy as jnp
from jax import lax
from jax.experimental import pallas as pl
from jax.experimental.pallas import tpu as pltpu
from jax.sharding import PartitionSpec as P

HD = 128
PAGE = 128
NEG = -1e30
FLOOR = -8192.0
SCALE2 = math.log2(math.e) / math.sqrt(HD)
LANES = 128
EXTRA = 16
DOCS = 4
COST = 10**8
CHUNK = 256


VMEM = pl.BlockSpec(memory_space=pltpu.VMEM)
SMEM = pl.BlockSpec(memory_space=pltpu.SMEM)


def scores_of(k, q):
    return (
        lax.dot_general(k, q, (((1,), (1,)), ((), ())), preferred_element_type=jnp.float32) * SCALE2
    )


def flipped(v):
    return jnp.concatenate([v.T, jnp.ones((EXTRA, v.shape[0]), v.dtype)], axis=0)


def doc_starts(doc_ref):
    ids = doc_ref[...]
    return [jnp.sum((ids < d).astype(jnp.int32)) for d in range(1, DOCS)]


def start_at(starts, position):
    start = jnp.zeros_like(position)
    for edge in starts:
        start = jnp.where(position >= edge, edge, start)
    return start


def attend_tile(q, keys, values, state, scratch, i, row_pos, docs, key_pos, win, first, diag, masked):
    m_ref, l_ref, acc_ref = state
    s_ref, p_ref = scratch
    heads = m_ref.shape[1]
    group = heads // len(keys)
    span = keys[0].shape[0]
    chunk = math.gcd(span, CHUNK)
    olds, freshes = {}, {}

    def score(h, c):
        part = slice(c, c + chunk)
        s = scores_of(keys[h // group][part, :], q(slice(h * HD, (h + 1) * HD)))
        if masked:
            if diag:
                allowed = (key_pos[part] >= docs) & (key_pos[part] <= row_pos)
            else:
                allowed = key_pos[part] >= jnp.maximum(docs, row_pos - win[h] + 1)
            s = jnp.where(allowed, s, NEG)
        s_ref[h, part, :] = s
        top = jnp.max(s.reshape(chunk // 8, 8, s.shape[1]), axis=0)
        freshes[h] = top if c == 0 else jnp.maximum(freshes[h], top)
        if c + chunk == span:
            top = jnp.max(freshes[h], axis=0, keepdims=True)
            if not first:
                olds[h] = m_ref[i, h : h + 1, :]
                top = jnp.maximum(olds[h], top)
            freshes[h] = top

    def weigh(h, c):
        part = slice(c, c + chunk)
        p_ref[h, part, :] = jnp.exp2(s_ref[h, part, :] - freshes[h]).astype(jnp.bfloat16)

    def gather(h):
        columns = slice(h * HD, (h + 1) * HD)
        pv = jnp.dot(values[h // group], p_ref[h, :span, :], preferred_element_type=jnp.float32)
        m_ref[i, h : h + 1, :] = freshes[h]
        if first:
            l_ref[i, h : h + 1, :] = pv[HD : HD + 1, :]
            acc_ref[i, columns, :] = pv[:HD, :]
        else:
            shrink = jnp.exp2(olds[h] - freshes[h])
            l_ref[i, h : h + 1, :] = l_ref[i, h : h + 1, :] * shrink + pv[HD : HD + 1, :]
            acc_ref[i, columns, :] = acc_ref[i, columns, :] * shrink + pv[:HD, :]

    for step in range(heads + 2):
        for c in range(0, span, chunk):
            if step < heads:
                score(step, c)
            if 0 <= step - 1 < heads:
                weigh(step - 1, c)
            if step >= 2 and c == 0:
                gather(step - 2)


def own_kernel(win, doc_ref, q_ref, k_ref, v_ref, info_ref, m_ref, l_ref, acc_ref, s_ref, p_ref):
    tiles, _, tq = m_ref.shape
    kv = k_ref.shape[1] // HD
    base = lax.axis_index("seq") * (tiles * tq)
    starts = doc_starts(doc_ref)
    for d, start in enumerate(starts):
        info_ref[d] = start
    whole = [flipped(v_ref[:, g * HD : (g + 1) * HD]) for g in range(kv)]
    for i in range(tiles):
        span = (i + 1) * tq
        row_pos = base + i * tq + lax.broadcasted_iota(jnp.int32, (1, tq), 1)
        key_pos = base + lax.broadcasted_iota(jnp.int32, (span, tq), 0)
        keys = [k_ref[:span, g * HD : (g + 1) * HD] for g in range(kv)]
        values = [v[:, :span] for v in whole]
        attend_tile(
            lambda columns, i=i: q_ref[i * tq : (i + 1) * tq, columns],
            keys, values, (m_ref, l_ref, acc_ref), (s_ref, p_ref), i,
            row_pos, start_at(starts, row_pos), key_pos, win, True, True, True,
        )


def far_kernel(win, info, *refs, sources, last):
    refs = list(refs)
    q_ref = refs[0]
    refs = refs[4:]
    blocks = []
    for distance in sources:
        blocks.append((distance, refs[0], refs[1]))
        refs = refs[2:]
    m_ref, l_ref, acc_ref = refs[:3]
    v_scratch, s_ref, p_ref = refs[-3:]
    out_ref = refs[3]
    tiles, heads, tq = m_ref.shape
    kv = blocks[0][2].shape[1] // HD
    seq = lax.axis_index("seq")
    base = seq * (tiles * tq)
    starts = [info[d] for d in range(DOCS - 1)]
    least, most = win[0], win[0]
    for h in range(1, heads):
        least, most = jnp.minimum(least, win[h]), jnp.maximum(most, win[h])
    for index, (_, _, v_ref) in enumerate(blocks):
        for g in range(kv):
            v_scratch[index, g] = flipped(v_ref[:, g * HD : (g + 1) * HD])

    def q_tile(i, _):
        first_row = base + i * tq
        last_row = first_row + tq - 1
        need_low = jnp.maximum(start_at(starts, first_row), first_row - most + 1)
        full_low = jnp.maximum(start_at(starts, last_row), last_row - least + 1)
        for index, (distance, k_ref, v_ref) in enumerate(blocks):
            span = v_ref.shape[0]
            key_base = base - distance * span
            needed = (key_base >= 0) & (key_base + span - 1 >= need_low)
            full = key_base >= full_low

            def body(masked, index=index, key_base=key_base, k_ref=k_ref, span=span):
                keys = [k_ref[:, g * HD : (g + 1) * HD] for g in range(kv)]
                values = [v_scratch[index, g] for g in range(kv)]
                row_pos = first_row + lax.broadcasted_iota(jnp.int32, (1, tq), 1)
                key_pos = key_base + lax.broadcasted_iota(jnp.int32, (span, tq), 0)
                attend_tile(
                    lambda columns: q_ref[pl.ds(pl.multiple_of(i * tq, tq), tq), columns],
                    keys, values, (m_ref, l_ref, acc_ref), (s_ref, p_ref), i,
                    row_pos, start_at(starts, row_pos) if masked else None, key_pos, win, False, False, masked,
                )

            pl.when(needed & full)(lambda body=body: body(False))
            pl.when(needed & jnp.logical_not(full))(lambda body=body: body(True))
        return 0

    lax.fori_loop(0, tiles, q_tile, 0)
    if last:
        half = lax.axis_index("tp")
        for i in range(tiles):
            place = pl.ds(pl.multiple_of(jnp.where(half == i, tq, 0), tq), tq)
            for h in range(heads):
                columns = slice(h * HD, (h + 1) * HD)
                value = acc_ref[i, columns, :] / l_ref[i, h : h + 1, :]
                out_ref[place, columns] = value.T.astype(jnp.bfloat16)


def decode_kernel(order, lengths, q_ref, ok_ref, ov_ref, k_ref, v_ref, out_ref, s_ref, *, per_request):
    requests = ok_ref.shape[0]
    group = q_ref.shape[1] // HD
    lanes = group * requests
    pages = k_ref.shape[0] // PAGE
    q = jnp.concatenate([q_ref[:, j * HD : (j + 1) * HD] for j in range(group)], axis=0)
    request = jnp.concatenate([lax.broadcasted_iota(jnp.int32, (1, requests), 1)] * group, axis=1)
    place = lax.broadcasted_iota(jnp.int32, (PAGE, lanes), 0)
    own = scores_of(ok_ref[...], q)
    own_row = lax.broadcasted_iota(jnp.int32, (requests, lanes), 0)
    own = jnp.where((own_row == request) & (lax.axis_index("seq") == 0), own, NEG)
    tops = jnp.max(own.reshape(requests // 8, 8, lanes), axis=0)
    for p in range(pages):
        s = scores_of(k_ref[p * PAGE : (p + 1) * PAGE, :], q)
        code = order[p]
        owner = code // per_request
        limit = lengths[owner] - (code - owner * per_request) * PAGE
        s = jnp.where(place < jnp.where(request == owner, limit, 0), s, NEG)
        s_ref[p * PAGE : (p + 1) * PAGE, :] = s
        tops = jnp.maximum(tops, jnp.max(s.reshape(PAGE // 8, 8, lanes), axis=0))
    top = jnp.max(tops, axis=0, keepdims=True)
    top = jnp.maximum(jnp.ceil(top * (1.0 / 32.0)) * 32.0, FLOOR)
    weights = jnp.exp2(s_ref[...] - top).astype(jnp.bfloat16)
    pv = jnp.dot(flipped(v_ref[...]), weights, preferred_element_type=jnp.float32)
    own_weights = jnp.exp2(own - top).astype(jnp.bfloat16)
    pv = pv + jnp.dot(flipped(ov_ref[...]), own_weights, preferred_element_type=jnp.float32)
    out_ref[:HD, :] = pv[:HD, :].astype(jnp.bfloat16)
    out_ref[HD:, :] = packed_stats(top, pv[HD : HD + 1, :])


def packed_stats(top, total):
    high = total.astype(jnp.bfloat16).astype(jnp.float32)
    row = lax.broadcasted_iota(jnp.int32, (EXTRA, top.shape[1]), 0)
    stats = jnp.where(row == 0, top, jnp.where(row == 1, high, total - high))
    return stats.astype(jnp.bfloat16)


def merge_kernel(a_ref, b_ref, out_ref, *, requests, last):
    rows, lanes = a_ref.shape
    kv = rows // (HD + EXTRA)
    group = lanes // requests
    f32 = jnp.float32
    for g in range(kv):
        base = g * (HD + EXTRA)
        body, tile = slice(base, base + HD), slice(base + HD, base + HD + EXTRA)
        left, right = a_ref[tile, :].astype(f32), b_ref[tile, :].astype(f32)
        top = jnp.maximum(left[0:1], right[0:1])
        e1, e2 = jnp.exp2(left[0:1] - top), jnp.exp2(right[0:1] - top)
        total = (left[1:2] + left[2:3]) * e1 + (right[1:2] + right[2:3]) * e2
        value = a_ref[body, :].astype(f32) * e1 + b_ref[body, :].astype(f32) * e2
        if not last:
            out_ref[body, :] = value.astype(jnp.bfloat16)
            out_ref[tile, :] = packed_stats(top, total)
            continue
        value = (value / total).T.astype(jnp.bfloat16)
        per = requests // 2
        half = lax.axis_index("tp")
        for j in range(group):
            columns = slice((g * group + j) * HD, (g * group + j + 1) * HD)
            for part in range(2):
                place = pl.ds(pl.multiple_of(jnp.where(half == part, per, 0), per), per)
                start = j * requests + part * per
                out_ref[place, columns] = value[start : start + per, :]


def product(x, w):
    return jnp.dot(x, w, preferred_element_type=jnp.float32).astype(jnp.bfloat16)


def project_kernel(a_ref, d_ref, w_ref, out_ref, *, column, second):
    x = half_rows(a_ref, d_ref, second)
    step = math.gcd(out_ref.shape[1], 512)
    for c in range(0, out_ref.shape[1], step):
        out_ref[:, c : c + step] = product(x, w_ref[:, column + c : column + c + step])


def half_rows(a_ref, d_ref, second):
    tr, dr = a_ref.shape[0] // 2, d_ref.shape[0] // 2
    return jnp.concatenate(
        [a_ref[second * tr : (second + 1) * tr, :], d_ref[second * dr : (second + 1) * dr, :]], axis=0
    )


def finish_kernel(a_ref, d_ref, w_ref, mine_ref, r0_ref, r1_ref, po_ref, do_ref, s_ref, sems):
    tr = po_ref.shape[0]
    early = mine_ref.shape[1]
    step = math.gcd(early, 512)
    x = half_rows(a_ref, d_ref, 1)
    copies = []
    for c in range(0, po_ref.shape[1], step):
        part = slice(c, c + step)
        if c < early:
            mine, other = mine_ref[:, part], r0_ref[:, part]
        else:
            mine, other = product(x, w_ref[:, part]), r1_ref[:, c - early : c - early + step]
        s_ref[:, part] = (mine.astype(jnp.float32) + other.astype(jnp.float32)).astype(jnp.bfloat16)
        slot = 2 * (c // step)
        copies.append(pltpu.make_async_copy(s_ref.at[:tr, part], po_ref.at[:, part], sems.at[slot]))
        copies.append(pltpu.make_async_copy(s_ref.at[tr:, part], do_ref.at[:, part], sems.at[slot + 1]))
        copies[-2].start()
        copies[-1].start()
    for copy in copies:
        copy.wait()


def on_device(
    prefill_query, prefill_key, prefill_value, doc_ids, head_window,
    dec_query, dec_key, dec_value, cache_key, cache_value, page_order, lengths, out_proj,
):
    n = lax.axis_size("seq")
    tokens, width = prefill_query.shape
    kv = prefill_key.shape[1] // HD
    heads = width // HD
    reach = n // 2
    tiles, tq = 2, tokens // 2
    odd = lax.axis_index("seq") % 2
    f32, bf16, i32 = jnp.float32, jnp.bfloat16, jnp.int32

    def line(x, by):
        return lax.ppermute(x, "seq", [(i, i + by) for i in range(n - by)])

    def swap(x, bit=1):
        return lax.ppermute(x, "seq", [(i, i ^ bit) for i in range(n)])

    def pick(even_value, odd_value):
        return jnp.where(odd == 1, odd_value, even_value)

    def params(mib):
        return pltpu.CompilerParams(vmem_limit_bytes=mib << 20)

    def cost(us):
        return pl.CostEstimate(flops=int(us * COST), transcendentals=0, bytes_accessed=1 << 20)

    pages = page_order.shape[0]
    requests = dec_query.shape[0]
    group = heads // kv
    tall = HD + EXTRA
    state = [
        jax.ShapeDtypeStruct((tiles, heads, tq), f32),
        jax.ShapeDtypeStruct((tiles, heads, tq), f32),
        jax.ShapeDtypeStruct((tiles, width, tq), f32),
    ]
    pair = [pltpu.VMEM((heads, tokens, tq), f32), pltpu.VMEM((heads, tokens, tq), bf16)]

    def decode_pages(order):
        return pl.pallas_call(
            lambda *refs: decode_kernel(*refs, per_request=pages * n // requests),
            grid=(kv,),
            in_specs=[
                SMEM, SMEM,
                pl.BlockSpec((requests, group * HD), lambda g: (0, g)),
                pl.BlockSpec((requests, HD), lambda g: (0, g)),
                pl.BlockSpec((requests, HD), lambda g: (0, g)),
                pl.BlockSpec((pages * PAGE, HD), lambda g: (0, g)),
                pl.BlockSpec((pages * PAGE, HD), lambda g: (0, g)),
            ],
            out_specs=pl.BlockSpec((tall, group * requests), lambda g: (g, 0)),
            out_shape=jax.ShapeDtypeStruct((kv * tall, group * requests), bf16),
            scratch_shapes=[pltpu.VMEM((pages * PAGE, group * requests), f32)],
            cost_estimate=cost(5),
            compiler_params=params(24),
            name="decode_pages",
        )(order, lengths, *[pltpu.with_memory_space_constraint(x, pltpu.HBM) for x in (dec_query, dec_key, dec_value, cache_key, cache_value)])

    def merge(partial, other, last):
        return pl.pallas_call(
            lambda *refs: merge_kernel(*refs, requests=requests, last=last),
            in_specs=[VMEM, VMEM],
            out_specs=VMEM,
            out_shape=jax.ShapeDtypeStruct((requests, width) if last else partial.shape, bf16),
            cost_estimate=cost(1),
            compiler_params=params(4),
            name="decode_merge",
        )(partial, other)

    def own(ids):
        return pl.pallas_call(
            own_kernel,
            in_specs=[SMEM] + [VMEM] * 4,
            out_specs=[SMEM] + [VMEM] * 3,
            out_shape=[jax.ShapeDtypeStruct((DOCS - 1,), i32)] + state,
            scratch_shapes=pair,
            cost_estimate=cost(3),
            compiler_params=params(16),
            name="prompt_own",
        )(head_window, ids.reshape(-1, LANES), prefill_query, prefill_key, prefill_value)

    def far(info, carry, stage, last):
        operands = [x for d in stage for x in (keys[d], values[d])]
        scratch = [pltpu.VMEM((len(stage), kv, tall, tokens), bf16)] + pair
        return pl.pallas_call(
            lambda *refs: far_kernel(*refs, sources=stage, last=last),
            in_specs=[SMEM, SMEM] + [VMEM] * (4 + len(operands)),
            out_specs=[VMEM] * (3 + last),
            out_shape=state + [jax.ShapeDtypeStruct((tokens, width), bf16)] * last,
            input_output_aliases={3: 0, 4: 1, 5: 2},
            scratch_shapes=scratch,
            cost_estimate=cost(5),
            compiler_params=params(20),
            name="prompt_far",
        )(head_window, info, prefill_query, *carry, *operands)

    token = [()]

    def then(x):
        x, *token[0] = lax.optimization_barrier((x, *token[0]))
        return x

    def done(*values):
        token[0] = list(values)
        return values if len(values) > 1 else values[0]

    keys, values = {0: prefill_key}, {0: prefill_value}

    def relay(table, d):
        table[d] = done(then(table[d]))
        if d < reach:
            table[d + 2] = line(table[d], 2)
        table[d - 1] = swap(done(pick(table[d - 2], table[d])))

    keys[2], values[2] = line(prefill_key, 2), line(prefill_value, 2)
    partial = done(decode_pages(page_order))
    other, bit = swap(partial), 2
    relay(keys, 2)
    info, *carry = done(*own(then(doc_ids)))
    relay(values, 2)

    def step(partial, other, bit):
        partial = done(merge(then(partial), other, bit >= n))
        return partial, (swap(partial, bit) if bit < n else None), bit * 2

    def attend(d):
        carry[0] = then(carry[0])
        carry[:] = far(info, carry[:3], (d,), d == reach - 1)
        done(carry[0])

    partial, other, bit = step(partial, other, bit)
    for d in range(4, reach + 1, 2):
        relay(keys, d)
        attend(d - 2)
        relay(values, d)
        attend(d - 3)
        if other is not None:
            partial, other, bit = step(partial, other, bit)
    attend(reach)
    while other is not None:
        partial, other, bit = step(partial, other, bit)
    attend(reach - 1)
    attn, decode_attn = carry[-1], partial

    model = out_proj.shape[1]
    tr, dr = tokens // 2, requests // 2
    cols = model // 2

    def project(column, second):
        return pl.pallas_call(
            lambda *refs: project_kernel(*refs, column=column, second=second),
            in_specs=[VMEM] * 3,
            out_specs=VMEM,
            out_shape=jax.ShapeDtypeStruct((tr + dr, cols), bf16),
            cost_estimate=cost(2),
            compiler_params=params(16),
            name="project_own" if second else "project_theirs",
        )(attn, decode_attn, out_proj)

    received = []
    for c in range(2):
        decode_attn = then(decode_attn)
        received.append(lax.ppermute(done(project(c * cols, 0)), "tp", [(0, 1), (1, 0)]))
    decode_attn = then(decode_attn)
    mine = project(0, 1)
    return tuple(
        pl.pallas_call(
            finish_kernel,
            in_specs=[VMEM] * 6,
            out_specs=[pl.BlockSpec(memory_space=pl.ANY)] * 2,
            out_shape=[jax.ShapeDtypeStruct((tr, model), bf16), jax.ShapeDtypeStruct((dr, model), bf16)],
            scratch_shapes=[
                pltpu.VMEM((tr + dr, model), bf16),
                pltpu.SemaphoreType.DMA((2 * (model // math.gcd(cols, 512)),)),
            ],
            cost_estimate=cost(3),
            compiler_params=params(20),
            name="project_finish",
        )(attn, decode_attn, out_proj, mine, *received)
    )


def solution(mesh):
    placed = (
        P(("rep", "seq"), "tp"),
        P(("rep", "seq"), "tp"),
        P(("rep", "seq"), "tp"),
        P("rep"),
        P("tp"),
        P("rep", "tp"),
        P("rep", "tp"),
        P("rep", "tp"),
        P(("rep", "seq"), "tp"),
        P(("rep", "seq"), "tp"),
        P(("rep", "seq")),
        P("rep"),
        P("tp", None),
    )
    return jax.shard_map(
        on_device,
        mesh=mesh,
        in_specs=placed,
        out_specs=(P(("rep", "seq", "tp"), None), P(("rep", "tp"), None)),
        check_vma=False,
    )
```

```python
import math

import jax
import jax.numpy as jnp
from jax import lax
from jax.experimental import pallas as pl
from jax.experimental.pallas import tpu as pltpu
from jax.sharding import PartitionSpec as P


HD = 128
PAGE = 128
NEG = -1e30
FLOOR = -8192.0
SCALE2 = math.log2(math.e) / math.sqrt(HD)
LANES = 128
EXTRA = 16
DOCS = 4
COST = 10**8
CHUNK = 256


VMEM = pl.BlockSpec(memory_space=pltpu.VMEM)
SMEM = pl.BlockSpec(memory_space=pltpu.SMEM)


def scores_of(k, q):
    return (
        lax.dot_general(k, q, (((1,), (1,)), ((), ())), preferred_element_type=jnp.float32) * SCALE2
    )


def flipped(v):
    return jnp.concatenate([v.T, jnp.ones((EXTRA, v.shape[0]), v.dtype)], axis=0)


def doc_starts(doc_ref):
    ids = doc_ref[...]
    return [jnp.sum((ids < d).astype(jnp.int32)) for d in range(1, DOCS)]


def start_at(starts, position):
    start = jnp.zeros_like(position)
    for edge in starts:
        start = jnp.where(position >= edge, edge, start)
    return start


def attend_tile(q, keys, values, state, scratch, i, row_pos, docs, key_pos, win, first, diag, masked):
    m_ref, l_ref, acc_ref = state
    s_ref, p_ref = scratch
    heads = m_ref.shape[1]
    group = heads // len(keys)
    span = keys[0].shape[0]
    chunk = math.gcd(span, CHUNK)
    olds, freshes = {}, {}

    def score(h, c):
        part = slice(c, c + chunk)
        s = scores_of(keys[h // group][part, :], q(slice(h * HD, (h + 1) * HD)))
        if masked:
            if diag:
                allowed = (key_pos[part] >= docs) & (key_pos[part] <= row_pos)
            else:
                allowed = key_pos[part] >= jnp.maximum(docs, row_pos - win[h] + 1)
            s = jnp.where(allowed, s, NEG)
        s_ref[h, part, :] = s
        top = jnp.max(s.reshape(chunk // 8, 8, s.shape[1]), axis=0)
        freshes[h] = top if c == 0 else jnp.maximum(freshes[h], top)
        if c + chunk == span:
            top = jnp.max(freshes[h], axis=0, keepdims=True)
            if not first:
                olds[h] = m_ref[i, h : h + 1, :]
                top = jnp.maximum(olds[h], top)
            freshes[h] = top

    def weigh(h, c):
        part = slice(c, c + chunk)
        p_ref[h, part, :] = jnp.exp2(s_ref[h, part, :] - freshes[h]).astype(jnp.bfloat16)

    def gather(h):
        columns = slice(h * HD, (h + 1) * HD)
        pv = jnp.dot(values[h // group], p_ref[h, :span, :], preferred_element_type=jnp.float32)
        m_ref[i, h : h + 1, :] = freshes[h]
        if first:
            l_ref[i, h : h + 1, :] = pv[HD : HD + 1, :]
            acc_ref[i, columns, :] = pv[:HD, :]
        else:
            shrink = jnp.exp2(olds[h] - freshes[h])
            l_ref[i, h : h + 1, :] = l_ref[i, h : h + 1, :] * shrink + pv[HD : HD + 1, :]
            acc_ref[i, columns, :] = acc_ref[i, columns, :] * shrink + pv[:HD, :]

    for step in range(heads + 2):
        for c in range(0, span, chunk):
            if step < heads:
                score(step, c)
            if 0 <= step - 1 < heads:
                weigh(step - 1, c)
            if step >= 2 and c == 0:
                gather(step - 2)


def own_kernel(win, doc_ref, q_ref, k_ref, v_ref, info_ref, m_ref, l_ref, acc_ref, s_ref, p_ref):
    tiles, _, tq = m_ref.shape
    kv = k_ref.shape[1] // HD
    base = lax.axis_index("seq") * (tiles * tq)
    starts = doc_starts(doc_ref)
    for d, start in enumerate(starts):
        info_ref[d] = start
    for h in range(win.shape[0]):
        info_ref[DOCS - 1 + h] = win[h]
    whole = [flipped(v_ref[:, g * HD : (g + 1) * HD]) for g in range(kv)]
    for i in range(tiles):
        span = (i + 1) * tq
        row_pos = base + i * tq + lax.broadcasted_iota(jnp.int32, (1, tq), 1)
        key_pos = base + lax.broadcasted_iota(jnp.int32, (span, tq), 0)
        keys = [k_ref[:span, g * HD : (g + 1) * HD] for g in range(kv)]
        values = [v[:, :span] for v in whole]
        attend_tile(
            lambda columns, i=i: q_ref[i * tq : (i + 1) * tq, columns],
            keys, values, (m_ref, l_ref, acc_ref), (s_ref, p_ref), i,
            row_pos, start_at(starts, row_pos), key_pos, win, True, True, True,
        )


def far_kernel(info, *refs, sources, last):
    refs = list(refs)
    q_ref = refs[0]
    refs = refs[4:]
    blocks = []
    for distance in sources:
        blocks.append((distance, refs[0], refs[1]))
        refs = refs[2:]
    m_ref, l_ref, acc_ref = refs[:3]
    v_scratch, s_ref, p_ref = refs[-3:]
    out_ref = refs[3]
    tiles, heads, tq = m_ref.shape
    kv = blocks[0][2].shape[1] // HD
    seq = lax.axis_index("seq")
    base = seq * (tiles * tq)
    starts = [info[d] for d in range(DOCS - 1)]
    win = [info[DOCS - 1 + h] for h in range(heads)]
    least, most = win[0], win[0]
    for h in range(1, heads):
        least, most = jnp.minimum(least, win[h]), jnp.maximum(most, win[h])
    for index, (_, _, v_ref) in enumerate(blocks):
        for g in range(kv):
            v_scratch[index, g] = flipped(v_ref[:, g * HD : (g + 1) * HD])

    def q_tile(i, _):
        first_row = base + i * tq
        last_row = first_row + tq - 1
        need_low = jnp.maximum(start_at(starts, first_row), first_row - most + 1)
        full_low = jnp.maximum(start_at(starts, last_row), last_row - least + 1)
        for index, (distance, k_ref, v_ref) in enumerate(blocks):
            span = v_ref.shape[0]
            key_base = base - distance * span
            needed = (key_base >= 0) & (key_base + span - 1 >= need_low)
            full = key_base >= full_low

            def body(masked, index=index, key_base=key_base, k_ref=k_ref, span=span):
                keys = [k_ref[:, g * HD : (g + 1) * HD] for g in range(kv)]
                values = [v_scratch[index, g] for g in range(kv)]
                row_pos = first_row + lax.broadcasted_iota(jnp.int32, (1, tq), 1)
                key_pos = key_base + lax.broadcasted_iota(jnp.int32, (span, tq), 0)
                attend_tile(
                    lambda columns: q_ref[pl.ds(pl.multiple_of(i * tq, tq), tq), columns],
                    keys, values, (m_ref, l_ref, acc_ref), (s_ref, p_ref), i,
                    row_pos, start_at(starts, row_pos) if masked else None, key_pos, win, False, False, masked,
                )

            pl.when(needed & full)(lambda body=body: body(False))
            pl.when(needed & jnp.logical_not(full))(lambda body=body: body(True))
        return 0

    lax.fori_loop(0, tiles, q_tile, 0)
    if last:
        half = lax.axis_index("tp")
        for i in range(tiles):
            place = pl.ds(pl.multiple_of(jnp.where(half == i, tq, 0), tq), tq)
            for h in range(heads):
                columns = slice(h * HD, (h + 1) * HD)
                value = acc_ref[i, columns, :] / l_ref[i, h : h + 1, :]
                out_ref[place, columns] = value.T.astype(jnp.bfloat16)


def decode_kernel(order, lengths, q_ref, ok_ref, ov_ref, k_ref, v_ref, out_ref, s_ref, *, per_request):
    requests = ok_ref.shape[0]
    group = q_ref.shape[1] // HD
    lanes = group * requests
    pages = k_ref.shape[0] // PAGE
    q = jnp.concatenate([q_ref[:, j * HD : (j + 1) * HD] for j in range(group)], axis=0)
    request = jnp.concatenate([lax.broadcasted_iota(jnp.int32, (1, requests), 1)] * group, axis=1)
    place = lax.broadcasted_iota(jnp.int32, (PAGE, lanes), 0)
    own = scores_of(ok_ref[...], q)
    own_row = lax.broadcasted_iota(jnp.int32, (requests, lanes), 0)
    own = jnp.where((own_row == request) & (lax.axis_index("seq") == 0), own, NEG)
    tops = jnp.max(own.reshape(requests // 8, 8, lanes), axis=0)
    for p in range(pages):
        s = scores_of(k_ref[p * PAGE : (p + 1) * PAGE, :], q)
        code = order[p]
        owner = code // per_request
        limit = lengths[owner] - (code - owner * per_request) * PAGE
        s = jnp.where(place < jnp.where(request == owner, limit, 0), s, NEG)
        s_ref[p * PAGE : (p + 1) * PAGE, :] = s
        tops = jnp.maximum(tops, jnp.max(s.reshape(PAGE // 8, 8, lanes), axis=0))
    top = jnp.max(tops, axis=0, keepdims=True)
    top = jnp.maximum(jnp.ceil(top * (1.0 / 32.0)) * 32.0, FLOOR)
    weights = jnp.exp2(s_ref[...] - top).astype(jnp.bfloat16)
    pv = jnp.dot(flipped(v_ref[...]), weights, preferred_element_type=jnp.float32)
    own_weights = jnp.exp2(own - top).astype(jnp.bfloat16)
    pv = pv + jnp.dot(flipped(ov_ref[...]), own_weights, preferred_element_type=jnp.float32)
    out_ref[:HD, :] = pv[:HD, :].astype(jnp.bfloat16)
    out_ref[HD:, :] = packed_stats(top, pv[HD : HD + 1, :])


def packed_stats(top, total):
    high = total.astype(jnp.bfloat16).astype(jnp.float32)
    row = lax.broadcasted_iota(jnp.int32, (EXTRA, top.shape[1]), 0)
    stats = jnp.where(row == 0, top, jnp.where(row == 1, high, total - high))
    return stats.astype(jnp.bfloat16)


def merge_kernel(a_ref, b_ref, out_ref, *, requests, last):
    rows, lanes = a_ref.shape
    kv = rows // (HD + EXTRA)
    group = lanes // requests
    f32 = jnp.float32
    for g in range(kv):
        base = g * (HD + EXTRA)
        body, tile = slice(base, base + HD), slice(base + HD, base + HD + EXTRA)
        left, right = a_ref[tile, :].astype(f32), b_ref[tile, :].astype(f32)
        top = jnp.maximum(left[0:1], right[0:1])
        e1, e2 = jnp.exp2(left[0:1] - top), jnp.exp2(right[0:1] - top)
        total = (left[1:2] + left[2:3]) * e1 + (right[1:2] + right[2:3]) * e2
        value = a_ref[body, :].astype(f32) * e1 + b_ref[body, :].astype(f32) * e2
        if not last:
            out_ref[body, :] = value.astype(jnp.bfloat16)
            out_ref[tile, :] = packed_stats(top, total)
            continue
        value = (value / total).T.astype(jnp.bfloat16)
        per = requests // 2
        half = lax.axis_index("tp")
        for j in range(group):
            columns = slice((g * group + j) * HD, (g * group + j + 1) * HD)
            for part in range(2):
                place = pl.ds(pl.multiple_of(jnp.where(half == part, per, 0), per), per)
                start = j * requests + part * per
                out_ref[place, columns] = value[start : start + per, :]


def product(x, w):
    return jnp.dot(x, w, preferred_element_type=jnp.float32).astype(jnp.bfloat16)


def project_kernel(a_ref, d_ref, w_ref, out_ref, *, column, second):
    x = half_rows(a_ref, d_ref, second)
    step = math.gcd(out_ref.shape[1], 512)
    for c in range(0, out_ref.shape[1], step):
        out_ref[:, c : c + step] = product(x, w_ref[:, column + c : column + c + step])


def half_rows(a_ref, d_ref, second):
    tr, dr = a_ref.shape[0] // 2, d_ref.shape[0] // 2
    return jnp.concatenate(
        [a_ref[second * tr : (second + 1) * tr, :], d_ref[second * dr : (second + 1) * dr, :]], axis=0
    )


def finish_kernel(*refs):
    po_ref, do_ref, s_ref, sems = refs[-4:]
    count = (len(refs) - 4) // 2
    tr = po_ref.shape[0]
    cols = refs[0].shape[1]
    copies = []
    for c in range(count):
        part = slice(c * cols, (c + 1) * cols)
        total = refs[c][...].astype(jnp.float32) + refs[count + c][...].astype(jnp.float32)
        s_ref[:, part] = total.astype(jnp.bfloat16)
        copies.append(pltpu.make_async_copy(s_ref.at[:tr, part], po_ref.at[:, part], sems.at[2 * c]))
        copies.append(pltpu.make_async_copy(s_ref.at[tr:, part], do_ref.at[:, part], sems.at[2 * c + 1]))
        copies[-2].start()
        copies[-1].start()
    for copy in copies:
        copy.wait()


def on_device(
    prefill_query, prefill_key, prefill_value, doc_ids, head_window,
    dec_query, dec_key, dec_value, cache_key, cache_value, page_order, lengths, out_proj,
):
    n = lax.axis_size("seq")
    tokens, width = prefill_query.shape
    kv = prefill_key.shape[1] // HD
    heads = width // HD
    reach = n // 2
    tiles, tq = 2, tokens // 2
    odd = lax.axis_index("seq") % 2
    f32, bf16, i32 = jnp.float32, jnp.bfloat16, jnp.int32

    def ring(x, by):
        return lax.ppermute(x, "seq", [(i, (i + by) % n) for i in range(n)])

    def swap(x, bit=1):
        return lax.ppermute(x, "seq", [(i, i ^ bit) for i in range(n)])

    def pick(even_value, odd_value):
        return jnp.where(odd == 1, odd_value, even_value)

    def params(mib):
        return pltpu.CompilerParams(vmem_limit_bytes=mib << 20)

    def hbm(*arrays):
        return [pltpu.with_memory_space_constraint(x, pltpu.HBM) for x in arrays]

    def cost(us):
        return pl.CostEstimate(flops=int(us * COST), transcendentals=0, bytes_accessed=1 << 20)

    pages = page_order.shape[0]
    requests = dec_query.shape[0]
    group = heads // kv
    tall = HD + EXTRA
    state = [
        jax.ShapeDtypeStruct((tiles, heads, tq), f32),
        jax.ShapeDtypeStruct((tiles, heads, tq), f32),
        jax.ShapeDtypeStruct((tiles, width, tq), f32),
    ]
    pair = [pltpu.VMEM((heads, tokens, tq), f32), pltpu.VMEM((heads, tokens, tq), bf16)]

    def decode_pages(order):
        return pl.pallas_call(
            lambda *refs: decode_kernel(*refs, per_request=pages * n // requests),
            grid=(kv,),
            in_specs=[
                SMEM, SMEM,
                pl.BlockSpec((requests, group * HD), lambda g: (0, g)),
                pl.BlockSpec((requests, HD), lambda g: (0, g)),
                pl.BlockSpec((requests, HD), lambda g: (0, g)),
                pl.BlockSpec((pages * PAGE, HD), lambda g: (0, g)),
                pl.BlockSpec((pages * PAGE, HD), lambda g: (0, g)),
            ],
            out_specs=pl.BlockSpec((tall, group * requests), lambda g: (g, 0)),
            out_shape=jax.ShapeDtypeStruct((kv * tall, group * requests), bf16),
            scratch_shapes=[pltpu.VMEM((pages * PAGE, group * requests), f32)],
            cost_estimate=cost(5),
            compiler_params=params(24),
            name="decode_pages",
        )(*hbm(order, lengths, dec_query, dec_key, dec_value, cache_key, cache_value))

    def merge(partial, other, last):
        return pl.pallas_call(
            lambda *refs: merge_kernel(*refs, requests=requests, last=last),
            in_specs=[VMEM, VMEM],
            out_specs=VMEM,
            out_shape=jax.ShapeDtypeStruct((requests, width) if last else partial.shape, bf16),
            cost_estimate=cost(1),
            compiler_params=params(4),
            name="decode_merge",
        )(partial, other)

    def own(ids):
        return pl.pallas_call(
            own_kernel,
            in_specs=[SMEM] + [VMEM] * 4,
            out_specs=[SMEM] + [VMEM] * 3,
            out_shape=[jax.ShapeDtypeStruct((DOCS - 1 + heads,), i32)] + state,
            scratch_shapes=pair,
            cost_estimate=cost(3),
            compiler_params=params(16),
            name="prompt_own",
        )(*hbm(head_window, ids.reshape(-1, LANES), prefill_query, prefill_key, prefill_value))

    def far(info, carry, stage, last):
        operands = [x for d in stage for x in (keys[d], values[d])]
        scratch = [pltpu.VMEM((len(stage), kv, tall, tokens), bf16)] + pair
        return pl.pallas_call(
            lambda *refs: far_kernel(*refs, sources=stage, last=last),
            in_specs=[SMEM] + [VMEM] * (4 + len(operands)),
            out_specs=[VMEM] * (3 + last),
            out_shape=state + [jax.ShapeDtypeStruct((tokens, width), bf16)] * last,
            input_output_aliases={2: 0, 3: 1, 4: 2},
            scratch_shapes=scratch,
            cost_estimate=cost(5),
            compiler_params=params(20),
            name="prompt_far",
        )(info, prefill_query, *carry, *operands)

    token = [()]

    def then(x):
        x, *token[0] = lax.optimization_barrier((x, *token[0]))
        return x

    def done(*values):
        token[0] = list(values)
        return values if len(values) > 1 else values[0]

    keys, values = {0: prefill_key}, {0: prefill_value}

    def relay(table, d):
        table[d] = done(then(table[d]))
        if d < reach:
            table[d + 2] = ring(table[d], 2)
        fresh = done(pick(table[d - 2], table[d]))
        table[d - 1] = swap(fresh)

    keys[2] = ring(prefill_key, 2)
    info, *carry = done(*own(doc_ids))
    values[2] = ring(then(prefill_value), 2)
    relay(keys, 2)
    partial = done(decode_pages(then(page_order)))
    relay(values, 2)
    other = swap(partial)
    bit = 2

    def step(partial, other, bit):
        partial = done(merge(then(partial), other, bit >= n))
        if bit >= n:
            return partial, None, bit
        return partial, swap(partial, bit), bit * 2

    def attend(d):
        carry[0] = then(carry[0])
        carry[:] = far(info, carry[:3], (d,), d == reach - 1)
        done(carry[0])

    for d in range(4, reach + 1, 2):
        relay(keys, d)
        if bit < n:
            partial, other, bit = step(partial, other, bit)
        relay(values, d)
        attend(d - 2)
        if bit < n:
            partial, other, bit = step(partial, other, bit)
        attend(d - 3)
    attend(reach)
    attend(reach - 1)
    while other is not None:
        partial, other, bit = step(partial, other, bit)
    attn, decode_attn = carry[-1], partial

    model = out_proj.shape[1]
    tr, dr = tokens // 2, requests // 2
    chunks = 2
    cols = model // chunks

    def project(column, second):
        return pl.pallas_call(
            lambda *refs: project_kernel(*refs, column=column, second=second),
            in_specs=[VMEM] * 3,
            out_specs=VMEM,
            out_shape=jax.ShapeDtypeStruct((tr + dr, cols), bf16),
            cost_estimate=cost(2),
            compiler_params=params(16),
            name="project_own" if second else "project_theirs",
        )(attn, decode_attn, out_proj)

    mine, received = [], []
    for c in range(chunks):
        sent = project(c * cols, 0)
        received.append(lax.ppermute(sent, "tp", [(0, 1), (1, 0)]))
        decode_attn = lax.optimization_barrier((decode_attn, sent))[0]
    for c in range(chunks):
        mine.append(project(c * cols, 1))
    return tuple(
        pl.pallas_call(
            finish_kernel,
            in_specs=[VMEM] * (2 * chunks),
            out_specs=[pl.BlockSpec(memory_space=pl.ANY)] * 2,
            out_shape=[jax.ShapeDtypeStruct((tr, model), bf16), jax.ShapeDtypeStruct((dr, model), bf16)],
            scratch_shapes=[pltpu.VMEM((tr + dr, model), bf16), pltpu.SemaphoreType.DMA((2 * chunks,))],
            cost_estimate=cost(3),
            compiler_params=params(12),
            name="project_finish",
        )(*mine, *received)
    )


def solution(mesh):
    placed = (
        P(("rep", "seq"), "tp"),
        P(("rep", "seq"), "tp"),
        P(("rep", "seq"), "tp"),
        P("rep"),
        P("tp"),
        P("rep", "tp"),
        P("rep", "tp"),
        P("rep", "tp"),
        P(("rep", "seq"), "tp"),
        P(("rep", "seq"), "tp"),
        P(("rep", "seq")),
        P("rep"),
        P("tp", None),
    )

    return jax.shard_map(
        on_device,
        mesh=mesh,
        in_specs=placed,
        out_specs=(P(("rep", "seq", "tp"), None), P(("rep", "tp"), None)),
        check_vma=False,
    )
```

```python
import math

import jax
import jax.numpy as jnp
from jax import lax
from jax.experimental import pallas as pl
from jax.experimental.pallas import tpu as pltpu
from jax.sharding import PartitionSpec as P


HD = 128
PAGE = 128
NEG = -1e30
FLOOR = -8192.0
SCALE2 = math.log2(math.e) / math.sqrt(HD)
LANES = 128
EXTRA = 16
DOCS = 4
COST = 10**8
CHUNK = 256


VMEM = pl.BlockSpec(memory_space=pltpu.VMEM)
SMEM = pl.BlockSpec(memory_space=pltpu.SMEM)


def scores_of(k, q):
    return (
        lax.dot_general(k, q, (((1,), (1,)), ((), ())), preferred_element_type=jnp.float32) * SCALE2
    )


def twice(k):
    return jnp.concatenate([k, k], axis=1)


def split_scaled(q):
    scaled = q.astype(jnp.float32).T * SCALE2
    high = scaled.astype(jnp.bfloat16)
    return jnp.concatenate([high, (scaled - high.astype(jnp.float32)).astype(jnp.bfloat16)], axis=0)


def flipped(v):
    return jnp.concatenate([v.T, jnp.ones((EXTRA, v.shape[0]), v.dtype)], axis=0)


def doc_starts(doc_ref):
    ids = doc_ref[...]
    return [jnp.sum((ids < d).astype(jnp.int32)) for d in range(1, DOCS)]


def start_at(starts, position):
    start = jnp.zeros_like(position)
    for edge in starts:
        start = jnp.where(position >= edge, edge, start)
    return start


def attend_tile(q_ref, keys, values, state, scratch, i, row_pos, docs, key_pos, win, first, diag, masked):
    m_ref, l_ref, acc_ref = state
    s_ref, p_ref = scratch
    heads = m_ref.shape[1]
    group = heads // len(keys)
    span = keys[0].shape[0]
    chunk = math.gcd(span, CHUNK)
    olds, freshes = {}, {}

    def score(h, c):
        part = slice(c, c + chunk)
        s = jnp.dot(
            keys[h // group][part, :],
            q_ref[i, 2 * h * HD : 2 * (h + 1) * HD, :],
            preferred_element_type=jnp.float32,
        )
        if masked:
            if diag:
                allowed = (key_pos[part] >= docs) & (key_pos[part] <= row_pos)
            else:
                allowed = key_pos[part] >= jnp.maximum(docs, row_pos - win[h] + 1)
            s = jnp.where(allowed, s, NEG)
        s_ref[h, part, :] = s
        top = jnp.max(s.reshape(chunk // 8, 8, s.shape[1]), axis=0)
        freshes[h] = top if c == 0 else jnp.maximum(freshes[h], top)
        if c + chunk == span:
            top = jnp.max(freshes[h], axis=0, keepdims=True)
            if not first:
                olds[h] = m_ref[i, h : h + 1, :]
                top = jnp.maximum(olds[h], top)
            freshes[h] = top

    def weigh(h, c):
        part = slice(c, c + chunk)
        p_ref[h, part, :] = jnp.exp2(s_ref[h, part, :] - freshes[h]).astype(jnp.bfloat16)

    def gather(h):
        columns = slice(h * HD, (h + 1) * HD)
        pv = jnp.dot(values[h // group], p_ref[h, :span, :], preferred_element_type=jnp.float32)
        m_ref[i, h : h + 1, :] = freshes[h]
        if first:
            l_ref[i, h : h + 1, :] = pv[HD : HD + 1, :]
            acc_ref[i, columns, :] = pv[:HD, :]
        else:
            shrink = jnp.exp2(olds[h] - freshes[h])
            l_ref[i, h : h + 1, :] = l_ref[i, h : h + 1, :] * shrink + pv[HD : HD + 1, :]
            acc_ref[i, columns, :] = acc_ref[i, columns, :] * shrink + pv[:HD, :]

    for step in range(heads + 3):
        for c in range(0, span, chunk):
            if step < heads:
                score(step, c)
            if 0 <= step - 1 < heads:
                weigh(step - 1, c)
            if step >= 3 and c == 0:
                gather(step - 3)


def own_kernel(win, doc_ref, q_ref, k_ref, v_ref, info_ref, m_ref, l_ref, acc_ref, q2_ref, s_ref, p_ref):
    tiles, _, tq = m_ref.shape
    kv = k_ref.shape[1] // HD
    base = lax.axis_index("seq") * (tiles * tq)
    starts = doc_starts(doc_ref)
    for d, start in enumerate(starts):
        info_ref[d] = start
    for h in range(win.shape[0]):
        info_ref[DOCS - 1 + h] = win[h]
    for i in range(tiles):
        for h in range(m_ref.shape[1]):
            q = q_ref[i * tq : (i + 1) * tq, h * HD : (h + 1) * HD]
            q2_ref[i, 2 * h * HD : 2 * (h + 1) * HD, :] = split_scaled(q)
    whole = [flipped(v_ref[:, g * HD : (g + 1) * HD]) for g in range(kv)]
    for i in range(tiles):
        span = (i + 1) * tq
        row_pos = base + i * tq + lax.broadcasted_iota(jnp.int32, (1, tq), 1)
        key_pos = base + lax.broadcasted_iota(jnp.int32, (span, tq), 0)
        keys = [twice(k_ref[:span, g * HD : (g + 1) * HD]) for g in range(kv)]
        values = [v[:, :span] for v in whole]
        attend_tile(
            q2_ref, keys, values, (m_ref, l_ref, acc_ref), (s_ref, p_ref), i,
            row_pos, start_at(starts, row_pos), key_pos, win, True, True, True,
        )


def far_kernel(info, *refs, sources, last):
    refs = list(refs)
    q_ref = refs[0]
    refs = refs[4:]
    blocks = []
    for distance in sources:
        blocks.append((distance, refs[0], refs[1]))
        refs = refs[2:]
    m_ref, l_ref, acc_ref = refs[:3]
    v_scratch, s_ref, p_ref = refs[-3:]
    out_ref = refs[3]
    tiles, heads, tq = m_ref.shape
    kv = blocks[0][2].shape[1] // HD
    seq = lax.axis_index("seq")
    base = seq * (tiles * tq)
    starts = [info[d] for d in range(DOCS - 1)]
    win = [info[DOCS - 1 + h] for h in range(heads)]
    least, most = win[0], win[0]
    for h in range(1, heads):
        least, most = jnp.minimum(least, win[h]), jnp.maximum(most, win[h])
    for index, (_, _, v_ref) in enumerate(blocks):
        for g in range(kv):
            v_scratch[index, g] = flipped(v_ref[:, g * HD : (g + 1) * HD])

    def q_tile(i, _):
        first_row = base + i * tq
        last_row = first_row + tq - 1
        need_low = jnp.maximum(start_at(starts, first_row), first_row - most + 1)
        full_low = jnp.maximum(start_at(starts, last_row), last_row - least + 1)
        for index, (distance, k_ref, v_ref) in enumerate(blocks):
            span = v_ref.shape[0]
            key_base = base - distance * span
            needed = (key_base >= 0) & (key_base + span - 1 >= need_low)
            full = key_base >= full_low

            def body(masked, index=index, key_base=key_base, k_ref=k_ref, span=span):
                keys = [twice(k_ref[:, g * HD : (g + 1) * HD]) for g in range(kv)]
                values = [v_scratch[index, g] for g in range(kv)]
                row_pos = first_row + lax.broadcasted_iota(jnp.int32, (1, tq), 1)
                key_pos = key_base + lax.broadcasted_iota(jnp.int32, (span, tq), 0)
                attend_tile(
                    q_ref, keys, values, (m_ref, l_ref, acc_ref), (s_ref, p_ref), i,
                    row_pos, start_at(starts, row_pos) if masked else None, key_pos, win, False, False, masked,
                )

            pl.when(needed & full)(lambda body=body: body(False))
            pl.when(needed & jnp.logical_not(full))(lambda body=body: body(True))
        return 0

    lax.fori_loop(0, tiles, q_tile, 0)
    if last:
        half = lax.axis_index("tp")
        for i in range(tiles):
            place = pl.ds(pl.multiple_of(jnp.where(half == i, tq, 0), tq), tq)
            for h in range(heads):
                columns = slice(h * HD, (h + 1) * HD)
                value = acc_ref[i, columns, :] / l_ref[i, h : h + 1, :]
                out_ref[place, columns] = value.T.astype(jnp.bfloat16)


def decode_kernel(order, lengths, q_ref, ok_ref, ov_ref, k_ref, v_ref, out_ref, s_ref, *, per_request):
    requests = ok_ref.shape[0]
    group = q_ref.shape[1] // HD
    lanes = group * requests
    pages = k_ref.shape[0] // PAGE
    q = jnp.concatenate([q_ref[:, j * HD : (j + 1) * HD] for j in range(group)], axis=0)
    request = jnp.concatenate([lax.broadcasted_iota(jnp.int32, (1, requests), 1)] * group, axis=1)
    place = lax.broadcasted_iota(jnp.int32, (PAGE, lanes), 0)
    own = scores_of(ok_ref[...], q)
    own_row = lax.broadcasted_iota(jnp.int32, (requests, lanes), 0)
    own = jnp.where((own_row == request) & (lax.axis_index("seq") == 0), own, NEG)
    tops = jnp.max(own.reshape(requests // 8, 8, lanes), axis=0)
    for p in range(pages):
        s = scores_of(k_ref[p * PAGE : (p + 1) * PAGE, :], q)
        code = order[p]
        owner = code // per_request
        limit = lengths[owner] - (code - owner * per_request) * PAGE
        s = jnp.where(place < jnp.where(request == owner, limit, 0), s, NEG)
        s_ref[p * PAGE : (p + 1) * PAGE, :] = s
        tops = jnp.maximum(tops, jnp.max(s.reshape(PAGE // 8, 8, lanes), axis=0))
    top = jnp.max(tops, axis=0, keepdims=True)
    top = jnp.maximum(jnp.ceil(top * (1.0 / 32.0)) * 32.0, FLOOR)
    weights = jnp.exp2(s_ref[...] - top).astype(jnp.bfloat16)
    pv = jnp.dot(flipped(v_ref[...]), weights, preferred_element_type=jnp.float32)
    own_weights = jnp.exp2(own - top).astype(jnp.bfloat16)
    pv = pv + jnp.dot(flipped(ov_ref[...]), own_weights, preferred_element_type=jnp.float32)
    out_ref[:HD, :] = pv[:HD, :].astype(jnp.bfloat16)
    out_ref[HD:, :] = packed_stats(top, pv[HD : HD + 1, :])


def packed_stats(top, total):
    high = total.astype(jnp.bfloat16).astype(jnp.float32)
    row = lax.broadcasted_iota(jnp.int32, (EXTRA, top.shape[1]), 0)
    stats = jnp.where(row == 0, top, jnp.where(row == 1, high, total - high))
    return stats.astype(jnp.bfloat16)


def merge_kernel(a_ref, b_ref, out_ref, *, requests, last):
    rows, lanes = a_ref.shape
    kv = rows // (HD + EXTRA)
    group = lanes // requests
    f32 = jnp.float32
    for g in range(kv):
        base = g * (HD + EXTRA)
        body, tile = slice(base, base + HD), slice(base + HD, base + HD + EXTRA)
        left, right = a_ref[tile, :].astype(f32), b_ref[tile, :].astype(f32)
        top = jnp.maximum(left[0:1], right[0:1])
        e1, e2 = jnp.exp2(left[0:1] - top), jnp.exp2(right[0:1] - top)
        total = (left[1:2] + left[2:3]) * e1 + (right[1:2] + right[2:3]) * e2
        value = a_ref[body, :].astype(f32) * e1 + b_ref[body, :].astype(f32) * e2
        if not last:
            out_ref[body, :] = value.astype(jnp.bfloat16)
            out_ref[tile, :] = packed_stats(top, total)
            continue
        value = (value / total).T.astype(jnp.bfloat16)
        per = requests // 2
        half = lax.axis_index("tp")
        for j in range(group):
            columns = slice((g * group + j) * HD, (g * group + j + 1) * HD)
            for part in range(2):
                place = pl.ds(pl.multiple_of(jnp.where(half == part, per, 0), per), per)
                start = j * requests + part * per
                out_ref[place, columns] = value[start : start + per, :]


def product(x, w):
    return jnp.dot(x, w, preferred_element_type=jnp.float32).astype(jnp.bfloat16)


def project_kernel(a_ref, d_ref, w_ref, out_ref, *, column, second):
    x = half_rows(a_ref, d_ref, second)
    step = math.gcd(out_ref.shape[1], 512)
    for c in range(0, out_ref.shape[1], step):
        out_ref[:, c : c + step] = product(x, w_ref[:, column + c : column + c + step])


def half_rows(a_ref, d_ref, second):
    tr, dr = a_ref.shape[0] // 2, d_ref.shape[0] // 2
    return jnp.concatenate(
        [a_ref[second * tr : (second + 1) * tr, :], d_ref[second * dr : (second + 1) * dr, :]], axis=0
    )


def finish_kernel(*refs):
    po_ref, do_ref, s_ref, sems = refs[-4:]
    count = (len(refs) - 4) // 2
    tr = po_ref.shape[0]
    cols = refs[0].shape[1]
    copies = []
    for c in range(count):
        part = slice(c * cols, (c + 1) * cols)
        total = refs[c][...].astype(jnp.float32) + refs[count + c][...].astype(jnp.float32)
        s_ref[:, part] = total.astype(jnp.bfloat16)
        copies.append(pltpu.make_async_copy(s_ref.at[:tr, part], po_ref.at[:, part], sems.at[2 * c]))
        copies.append(pltpu.make_async_copy(s_ref.at[tr:, part], do_ref.at[:, part], sems.at[2 * c + 1]))
        copies[-2].start()
        copies[-1].start()
    for copy in copies:
        copy.wait()


def on_device(
    prefill_query, prefill_key, prefill_value, doc_ids, head_window,
    dec_query, dec_key, dec_value, cache_key, cache_value, page_order, lengths, out_proj,
):
    n = lax.axis_size("seq")
    tokens, width = prefill_query.shape
    kv = prefill_key.shape[1] // HD
    heads = width // HD
    reach = n // 2
    tiles, tq = 2, tokens // 2
    odd = lax.axis_index("seq") % 2
    f32, bf16, i32 = jnp.float32, jnp.bfloat16, jnp.int32

    def ring(x, by):
        return lax.ppermute(x, "seq", [(i, (i + by) % n) for i in range(n)])

    def swap(x, bit=1):
        return lax.ppermute(x, "seq", [(i, i ^ bit) for i in range(n)])

    def pick(even_value, odd_value):
        return jnp.where(odd == 1, odd_value, even_value)

    def params(mib):
        return pltpu.CompilerParams(vmem_limit_bytes=mib << 20)

    def hbm(*arrays):
        return [pltpu.with_memory_space_constraint(x, pltpu.HBM) for x in arrays]

    def cost(us):
        return pl.CostEstimate(flops=int(us * COST), transcendentals=0, bytes_accessed=1 << 20)

    pages = page_order.shape[0]
    requests = dec_query.shape[0]
    group = heads // kv
    tall = HD + EXTRA
    state = [
        jax.ShapeDtypeStruct((tiles, heads, tq), f32),
        jax.ShapeDtypeStruct((tiles, heads, tq), f32),
        jax.ShapeDtypeStruct((tiles, width, tq), f32),
    ]
    pair = [pltpu.VMEM((heads, tokens, tq), f32), pltpu.VMEM((heads, tokens, tq), bf16)]

    def decode_pages(order):
        return pl.pallas_call(
            lambda *refs: decode_kernel(*refs, per_request=pages * n // requests),
            grid=(kv,),
            in_specs=[
                SMEM, SMEM,
                pl.BlockSpec((requests, group * HD), lambda g: (0, g)),
                pl.BlockSpec((requests, HD), lambda g: (0, g)),
                pl.BlockSpec((requests, HD), lambda g: (0, g)),
                pl.BlockSpec((pages * PAGE, HD), lambda g: (0, g)),
                pl.BlockSpec((pages * PAGE, HD), lambda g: (0, g)),
            ],
            out_specs=pl.BlockSpec((tall, group * requests), lambda g: (g, 0)),
            out_shape=jax.ShapeDtypeStruct((kv * tall, group * requests), bf16),
            scratch_shapes=[pltpu.VMEM((pages * PAGE, group * requests), f32)],
            cost_estimate=cost(5),
            compiler_params=params(24),
            name="decode_pages",
        )(*hbm(order, lengths, dec_query, dec_key, dec_value, cache_key, cache_value))

    def merge(partial, other, last):
        return pl.pallas_call(
            lambda *refs: merge_kernel(*refs, requests=requests, last=last),
            in_specs=[VMEM, VMEM],
            out_specs=VMEM,
            out_shape=jax.ShapeDtypeStruct((requests, width) if last else partial.shape, bf16),
            cost_estimate=cost(1),
            compiler_params=params(4),
            name="decode_merge",
        )(partial, other)

    def own(ids):
        return pl.pallas_call(
            own_kernel,
            in_specs=[SMEM] + [VMEM] * 4,
            out_specs=[SMEM] + [VMEM] * 4,
            out_shape=[
                jax.ShapeDtypeStruct((DOCS - 1 + heads,), i32),
                *state,
                jax.ShapeDtypeStruct((tiles, 2 * width, tq), bf16),
            ],
            scratch_shapes=pair,
            cost_estimate=cost(3),
            compiler_params=params(16),
            name="prompt_own",
        )(*hbm(head_window, ids.reshape(-1, LANES), prefill_query, prefill_key, prefill_value))

    def far(info, queries, carry, stage, last):
        operands = [x for d in stage for x in (keys[d], values[d])]
        scratch = [pltpu.VMEM((len(stage), kv, tall, tokens), bf16)] + pair
        return pl.pallas_call(
            lambda *refs: far_kernel(*refs, sources=stage, last=last),
            in_specs=[SMEM] + [VMEM] * (4 + len(operands)),
            out_specs=[VMEM] * (3 + last),
            out_shape=state + [jax.ShapeDtypeStruct((tokens, width), bf16)] * last,
            input_output_aliases={2: 0, 3: 1, 4: 2},
            scratch_shapes=scratch,
            cost_estimate=cost(5),
            compiler_params=params(20),
            name="prompt_far",
        )(info, queries, *carry, *operands)

    token = [()]

    def then(x):
        x, *token[0] = lax.optimization_barrier((x, *token[0]))
        return x

    def done(*values):
        token[0] = list(values)
        return values if len(values) > 1 else values[0]

    keys, values = {0: prefill_key}, {0: prefill_value}

    def relay(table, d):
        table[d] = done(then(table[d]))
        if d < reach:
            table[d + 2] = ring(table[d], 2)
        fresh = done(pick(table[d - 2], table[d]))
        table[d - 1] = swap(fresh)

    keys[2] = ring(prefill_key, 2)
    partial = done(decode_pages(page_order))
    other = swap(partial)
    values[2] = ring(prefill_value, 2)
    relay(keys, 2)
    info, *carry, queries = done(*own(then(doc_ids)))
    relay(values, 2)
    bit = 2

    def step(partial, other, bit):
        partial = done(merge(then(partial), other, bit >= n))
        if bit >= n:
            return partial, None, bit
        return partial, swap(partial, bit), bit * 2

    def attend(*stage):
        carry[0] = then(carry[0])
        carry[:] = far(info, queries, carry[:3], stage, stage[-1] == reach - 1)
        done(carry[0])

    partial, other, bit = step(partial, other, bit)
    for d in range(4, reach + 1, 2):
        relay(keys, d)
        attend(d - 2)
        relay(values, d)
        if bit < n:
            partial, other, bit = step(partial, other, bit)
        attend(d - 3)
    attend(reach, reach - 1)
    while other is not None:
        partial, other, bit = step(partial, other, bit)
    attn, decode_attn = carry[-1], partial

    model = out_proj.shape[1]
    tr, dr = tokens // 2, requests // 2
    chunks = 2
    cols = model // chunks

    def project(column, second):
        return pl.pallas_call(
            lambda *refs: project_kernel(*refs, column=column, second=second),
            in_specs=[VMEM] * 3,
            out_specs=VMEM,
            out_shape=jax.ShapeDtypeStruct((tr + dr, cols), bf16),
            cost_estimate=cost(2),
            compiler_params=params(16),
            name="project_own" if second else "project_theirs",
        )(attn, decode_attn, out_proj)

    mine, received = [], []
    for c in range(chunks):
        sent = project(c * cols, 0)
        received.append(lax.ppermute(sent, "tp", [(0, 1), (1, 0)]))
        decode_attn = lax.optimization_barrier((decode_attn, sent))[0]
    for c in range(chunks):
        mine.append(project(c * cols, 1))
    return tuple(
        pl.pallas_call(
            finish_kernel,
            in_specs=[VMEM] * (2 * chunks),
            out_specs=[pl.BlockSpec(memory_space=pl.ANY)] * 2,
            out_shape=[jax.ShapeDtypeStruct((tr, model), bf16), jax.ShapeDtypeStruct((dr, model), bf16)],
            scratch_shapes=[pltpu.VMEM((tr + dr, model), bf16), pltpu.SemaphoreType.DMA((2 * chunks,))],
            cost_estimate=cost(3),
            compiler_params=params(12),
            name="project_finish",
        )(*mine, *received)
    )


def solution(mesh):
    placed = (
        P(("rep", "seq"), "tp"),
        P(("rep", "seq"), "tp"),
        P(("rep", "seq"), "tp"),
        P("rep"),
        P("tp"),
        P("rep", "tp"),
        P("rep", "tp"),
        P("rep", "tp"),
        P(("rep", "seq"), "tp"),
        P(("rep", "seq"), "tp"),
        P(("rep", "seq")),
        P("rep"),
        P("tp", None),
    )

    return jax.shard_map(
        on_device,
        mesh=mesh,
        in_specs=placed,
        out_specs=(P(("rep", "seq", "tp"), None), P(("rep", "tp"), None)),
        check_vma=False,
    )
```

```python
import math

import jax
import jax.numpy as jnp
from jax import lax
from jax.experimental import pallas as pl
from jax.experimental.pallas import tpu as pltpu
from jax.sharding import PartitionSpec as P


HD = 128
PAGE = 128
NEG = -1e30
FLOOR = -8192.0
SCALE2 = math.log2(math.e) / math.sqrt(HD)
LANES = 128
EXTRA = 16
DOCS = 4
COST = 10**8
CHUNK = 256


VMEM = pl.BlockSpec(memory_space=pltpu.VMEM)
SMEM = pl.BlockSpec(memory_space=pltpu.SMEM)


def scores_of(k, q):
    return (
        lax.dot_general(k, q, (((1,), (1,)), ((), ())), preferred_element_type=jnp.float32) * SCALE2
    )


def twice(k):
    return jnp.concatenate([k, k], axis=1)


def split_scaled(q):
    scaled = q.astype(jnp.float32).T * SCALE2
    high = scaled.astype(jnp.bfloat16)
    return jnp.concatenate([high, (scaled - high.astype(jnp.float32)).astype(jnp.bfloat16)], axis=0)


def flipped(v):
    return jnp.concatenate([v.T, jnp.ones((EXTRA, v.shape[0]), v.dtype)], axis=0)


def doc_starts(doc_ref):
    ids = doc_ref[...]
    return [jnp.sum((ids < d).astype(jnp.int32)) for d in range(1, DOCS)]


def start_at(starts, position):
    start = jnp.zeros_like(position)
    for edge in starts:
        start = jnp.where(position >= edge, edge, start)
    return start


def attend_tile(q_ref, keys, values, state, scratch, i, row_pos, docs, key_pos, win, first, diag, masked):
    m_ref, l_ref, acc_ref = state
    s_ref, p_ref = scratch
    heads = m_ref.shape[1]
    group = heads // len(keys)
    span = keys[0].shape[0]
    chunk = math.gcd(span, CHUNK)
    olds, freshes = {}, {}

    def score(h, c):
        part = slice(c, c + chunk)
        s = jnp.dot(
            keys[h // group][part, :],
            q_ref[i, 2 * h * HD : 2 * (h + 1) * HD, :],
            preferred_element_type=jnp.float32,
        )
        if masked:
            if diag:
                allowed = (key_pos[part] >= docs) & (key_pos[part] <= row_pos)
            else:
                allowed = key_pos[part] >= jnp.maximum(docs, row_pos - win[h] + 1)
            s = jnp.where(allowed, s, NEG)
        s_ref[h, part, :] = s
        top = jnp.max(s.reshape(chunk // 8, 8, s.shape[1]), axis=0)
        freshes[h] = top if c == 0 else jnp.maximum(freshes[h], top)
        if c + chunk == span:
            top = jnp.max(freshes[h], axis=0, keepdims=True)
            if not first:
                olds[h] = m_ref[i, h : h + 1, :]
                top = jnp.maximum(olds[h], top)
            freshes[h] = top

    def weigh(h, c):
        part = slice(c, c + chunk)
        p_ref[h, part, :] = jnp.exp2(s_ref[h, part, :] - freshes[h]).astype(jnp.bfloat16)

    def gather(h):
        columns = slice(h * HD, (h + 1) * HD)
        pv = jnp.dot(values[h // group], p_ref[h, :span, :], preferred_element_type=jnp.float32)
        m_ref[i, h : h + 1, :] = freshes[h]
        if first:
            l_ref[i, h : h + 1, :] = pv[HD : HD + 1, :]
            acc_ref[i, columns, :] = pv[:HD, :]
        else:
            shrink = jnp.exp2(olds[h] - freshes[h])
            l_ref[i, h : h + 1, :] = l_ref[i, h : h + 1, :] * shrink + pv[HD : HD + 1, :]
            acc_ref[i, columns, :] = acc_ref[i, columns, :] * shrink + pv[:HD, :]

    for step in range(heads + 3):
        for c in range(0, span, chunk):
            if step < heads:
                score(step, c)
            if 0 <= step - 1 < heads:
                weigh(step - 1, c)
            if step >= 3 and c == 0:
                gather(step - 3)


def own_kernel(win, doc_ref, q_ref, k_ref, v_ref, info_ref, m_ref, l_ref, acc_ref, q2_ref, s_ref, p_ref):
    tiles, _, tq = m_ref.shape
    kv = k_ref.shape[1] // HD
    base = lax.axis_index("seq") * (tiles * tq)
    starts = doc_starts(doc_ref)
    for d, start in enumerate(starts):
        info_ref[d] = start
    for h in range(win.shape[0]):
        info_ref[DOCS - 1 + h] = win[h]
    for i in range(tiles):
        for h in range(m_ref.shape[1]):
            q = q_ref[i * tq : (i + 1) * tq, h * HD : (h + 1) * HD]
            q2_ref[i, 2 * h * HD : 2 * (h + 1) * HD, :] = split_scaled(q)
    whole = [flipped(v_ref[:, g * HD : (g + 1) * HD]) for g in range(kv)]
    for i in range(tiles):
        span = (i + 1) * tq
        row_pos = base + i * tq + lax.broadcasted_iota(jnp.int32, (1, tq), 1)
        key_pos = base + lax.broadcasted_iota(jnp.int32, (span, tq), 0)
        keys = [twice(k_ref[:span, g * HD : (g + 1) * HD]) for g in range(kv)]
        values = [v[:, :span] for v in whole]
        attend_tile(
            q2_ref, keys, values, (m_ref, l_ref, acc_ref), (s_ref, p_ref), i,
            row_pos, start_at(starts, row_pos), key_pos, win, True, True, True,
        )


def far_kernel(info, *refs, sources, last):
    refs = list(refs)
    q_ref = refs[0]
    refs = refs[4:]
    blocks = []
    for distance in sources:
        blocks.append((distance, refs[0], refs[1]))
        refs = refs[2:]
    m_ref, l_ref, acc_ref = refs[:3]
    v_scratch, s_ref, p_ref = refs[-3:]
    out_ref = refs[3]
    tiles, heads, tq = m_ref.shape
    kv = blocks[0][2].shape[1] // HD
    seq = lax.axis_index("seq")
    base = seq * (tiles * tq)
    starts = [info[d] for d in range(DOCS - 1)]
    win = [info[DOCS - 1 + h] for h in range(heads)]
    least, most = win[0], win[0]
    for h in range(1, heads):
        least, most = jnp.minimum(least, win[h]), jnp.maximum(most, win[h])
    for index, (_, _, v_ref) in enumerate(blocks):
        for g in range(kv):
            v_scratch[index, g] = flipped(v_ref[:, g * HD : (g + 1) * HD])

    def q_tile(i, _):
        first_row = base + i * tq
        last_row = first_row + tq - 1
        need_low = jnp.maximum(start_at(starts, first_row), first_row - most + 1)
        full_low = jnp.maximum(start_at(starts, last_row), last_row - least + 1)
        for index, (distance, k_ref, v_ref) in enumerate(blocks):
            span = v_ref.shape[0]
            key_base = base - distance * span
            needed = (key_base >= 0) & (key_base + span - 1 >= need_low)
            full = key_base >= full_low

            def body(masked, index=index, key_base=key_base, k_ref=k_ref, span=span):
                keys = [twice(k_ref[:, g * HD : (g + 1) * HD]) for g in range(kv)]
                values = [v_scratch[index, g] for g in range(kv)]
                row_pos = first_row + lax.broadcasted_iota(jnp.int32, (1, tq), 1)
                key_pos = key_base + lax.broadcasted_iota(jnp.int32, (span, tq), 0)
                attend_tile(
                    q_ref, keys, values, (m_ref, l_ref, acc_ref), (s_ref, p_ref), i,
                    row_pos, start_at(starts, row_pos) if masked else None, key_pos, win, False, False, masked,
                )

            pl.when(needed & full)(lambda body=body: body(False))
            pl.when(needed & jnp.logical_not(full))(lambda body=body: body(True))
        return 0

    lax.fori_loop(0, tiles, q_tile, 0)
    if last:
        half = lax.axis_index("tp")
        for i in range(tiles):
            place = pl.ds(pl.multiple_of(jnp.where(half == i, tq, 0), tq), tq)
            for h in range(heads):
                columns = slice(h * HD, (h + 1) * HD)
                value = acc_ref[i, columns, :] / l_ref[i, h : h + 1, :]
                out_ref[place, columns] = value.T.astype(jnp.bfloat16)


def decode_kernel(order, lengths, q_ref, ok_ref, ov_ref, k_ref, v_ref, out_ref, s_ref, *, per_request):
    requests = ok_ref.shape[0]
    group = q_ref.shape[1] // HD
    lanes = group * requests
    pages = k_ref.shape[0] // PAGE
    q = jnp.concatenate([q_ref[:, j * HD : (j + 1) * HD] for j in range(group)], axis=0)
    request = jnp.concatenate([lax.broadcasted_iota(jnp.int32, (1, requests), 1)] * group, axis=1)
    place = lax.broadcasted_iota(jnp.int32, (PAGE, lanes), 0)
    own = scores_of(ok_ref[...], q)
    own_row = lax.broadcasted_iota(jnp.int32, (requests, lanes), 0)
    own = jnp.where((own_row == request) & (lax.axis_index("seq") == 0), own, NEG)
    tops = jnp.max(own.reshape(requests // 8, 8, lanes), axis=0)
    for p in range(pages):
        s = scores_of(k_ref[p * PAGE : (p + 1) * PAGE, :], q)
        code = order[p]
        owner = code // per_request
        limit = lengths[owner] - (code - owner * per_request) * PAGE
        s = jnp.where(place < jnp.where(request == owner, limit, 0), s, NEG)
        s_ref[p * PAGE : (p + 1) * PAGE, :] = s
        tops = jnp.maximum(tops, jnp.max(s.reshape(PAGE // 8, 8, lanes), axis=0))
    top = jnp.max(tops, axis=0, keepdims=True)
    top = jnp.maximum(jnp.ceil(top * (1.0 / 32.0)) * 32.0, FLOOR)
    weights = jnp.exp2(s_ref[...] - top).astype(jnp.bfloat16)
    pv = jnp.dot(flipped(v_ref[...]), weights, preferred_element_type=jnp.float32)
    own_weights = jnp.exp2(own - top).astype(jnp.bfloat16)
    pv = pv + jnp.dot(flipped(ov_ref[...]), own_weights, preferred_element_type=jnp.float32)
    out_ref[:HD, :] = pv[:HD, :].astype(jnp.bfloat16)
    out_ref[HD:, :] = packed_stats(top, pv[HD : HD + 1, :])


def packed_stats(top, total):
    high = total.astype(jnp.bfloat16).astype(jnp.float32)
    row = lax.broadcasted_iota(jnp.int32, (EXTRA, top.shape[1]), 0)
    stats = jnp.where(row == 0, top, jnp.where(row == 1, high, total - high))
    return stats.astype(jnp.bfloat16)


def merge_kernel(a_ref, b_ref, out_ref, *, requests, last):
    rows, lanes = a_ref.shape
    kv = rows // (HD + EXTRA)
    group = lanes // requests
    f32 = jnp.float32
    for g in range(kv):
        base = g * (HD + EXTRA)
        body, tile = slice(base, base + HD), slice(base + HD, base + HD + EXTRA)
        left, right = a_ref[tile, :].astype(f32), b_ref[tile, :].astype(f32)
        top = jnp.maximum(left[0:1], right[0:1])
        e1, e2 = jnp.exp2(left[0:1] - top), jnp.exp2(right[0:1] - top)
        total = (left[1:2] + left[2:3]) * e1 + (right[1:2] + right[2:3]) * e2
        value = a_ref[body, :].astype(f32) * e1 + b_ref[body, :].astype(f32) * e2
        if not last:
            out_ref[body, :] = value.astype(jnp.bfloat16)
            out_ref[tile, :] = packed_stats(top, total)
            continue
        value = (value / total).T.astype(jnp.bfloat16)
        per = requests // 2
        half = lax.axis_index("tp")
        for j in range(group):
            columns = slice((g * group + j) * HD, (g * group + j + 1) * HD)
            for part in range(2):
                place = pl.ds(pl.multiple_of(jnp.where(half == part, per, 0), per), per)
                start = j * requests + part * per
                out_ref[place, columns] = value[start : start + per, :]


def product(x, w):
    return jnp.dot(x, w, preferred_element_type=jnp.float32).astype(jnp.bfloat16)


def project_kernel(a_ref, d_ref, w_ref, out_ref, *, column, second):
    x = half_rows(a_ref, d_ref, second)
    step = math.gcd(out_ref.shape[1], 512)
    for c in range(0, out_ref.shape[1], step):
        out_ref[:, c : c + step] = product(x, w_ref[:, column + c : column + c + step])


def half_rows(a_ref, d_ref, second):
    tr, dr = a_ref.shape[0] // 2, d_ref.shape[0] // 2
    return jnp.concatenate(
        [a_ref[second * tr : (second + 1) * tr, :], d_ref[second * dr : (second + 1) * dr, :]], axis=0
    )


def emit(mine, other, s_ref, sems, outs, column):
    po_ref, do_ref = outs
    tr, cols = po_ref.shape[0], s_ref.shape[1]
    size = cols // 2
    copies = []
    for c in range(2):
        here, there = pl.ds(c * size, size), pl.ds(column + c * size, size)
        total = mine[:, here].astype(jnp.float32) + other[:, here].astype(jnp.float32)
        s_ref[:, here] = total.astype(jnp.bfloat16)
        copies.append(pltpu.make_async_copy(s_ref.at[:tr, here], po_ref.at[:, there], sems.at[2 * c]))
        copies.append(pltpu.make_async_copy(s_ref.at[tr:, here], do_ref.at[:, there], sems.at[2 * c + 1]))
        copies[-2].start()
        copies[-1].start()
    return copies


def early_kernel(a_ref, d_ref, w_ref, mine_ref, r_ref, po_ref, do_ref, next_ref, s_ref, sems):
    copies = emit(mine_ref, r_ref, s_ref, sems, (po_ref, do_ref), 0)
    project_kernel(a_ref, d_ref, w_ref, next_ref, column=mine_ref.shape[1], second=1)
    for copy in copies:
        copy.wait()


def late_kernel(mine_ref, r_ref, _po, _do, po_ref, do_ref, s_ref, sems):
    for copy in emit(mine_ref, r_ref, s_ref, sems, (po_ref, do_ref), mine_ref.shape[1]):
        copy.wait()


def on_device(
    prefill_query, prefill_key, prefill_value, doc_ids, head_window,
    dec_query, dec_key, dec_value, cache_key, cache_value, page_order, lengths, out_proj,
):
    n = lax.axis_size("seq")
    tokens, width = prefill_query.shape
    kv = prefill_key.shape[1] // HD
    heads = width // HD
    reach = n // 2
    tiles, tq = 2, tokens // 2
    odd = lax.axis_index("seq") % 2
    f32, bf16, i32 = jnp.float32, jnp.bfloat16, jnp.int32

    def ring(x, by):
        return lax.ppermute(x, "seq", [(i, (i + by) % n) for i in range(n)])

    def swap(x, bit=1):
        return lax.ppermute(x, "seq", [(i, i ^ bit) for i in range(n)])

    def pick(even_value, odd_value):
        return jnp.where(odd == 1, odd_value, even_value)

    def params(mib):
        return pltpu.CompilerParams(vmem_limit_bytes=mib << 20)

    def hbm(*arrays):
        return [pltpu.with_memory_space_constraint(x, pltpu.HBM) for x in arrays]

    def cost(us):
        return pl.CostEstimate(flops=int(us * COST), transcendentals=0, bytes_accessed=1 << 20)

    pages = page_order.shape[0]
    requests = dec_query.shape[0]
    group = heads // kv
    tall = HD + EXTRA
    state = [
        jax.ShapeDtypeStruct((tiles, heads, tq), f32),
        jax.ShapeDtypeStruct((tiles, heads, tq), f32),
        jax.ShapeDtypeStruct((tiles, width, tq), f32),
    ]
    pair = [pltpu.VMEM((heads, tokens, tq), f32), pltpu.VMEM((heads, tokens, tq), bf16)]

    def decode_pages(order):
        return pl.pallas_call(
            lambda *refs: decode_kernel(*refs, per_request=pages * n // requests),
            grid=(kv,),
            in_specs=[
                SMEM, SMEM,
                pl.BlockSpec((requests, group * HD), lambda g: (0, g)),
                pl.BlockSpec((requests, HD), lambda g: (0, g)),
                pl.BlockSpec((requests, HD), lambda g: (0, g)),
                pl.BlockSpec((pages * PAGE, HD), lambda g: (0, g)),
                pl.BlockSpec((pages * PAGE, HD), lambda g: (0, g)),
            ],
            out_specs=pl.BlockSpec((tall, group * requests), lambda g: (g, 0)),
            out_shape=jax.ShapeDtypeStruct((kv * tall, group * requests), bf16),
            scratch_shapes=[pltpu.VMEM((pages * PAGE, group * requests), f32)],
            cost_estimate=cost(5),
            compiler_params=params(24),
            name="decode_pages",
        )(*hbm(order, lengths, dec_query, dec_key, dec_value, cache_key, cache_value))

    def merge(partial, other, last):
        return pl.pallas_call(
            lambda *refs: merge_kernel(*refs, requests=requests, last=last),
            in_specs=[VMEM, VMEM],
            out_specs=VMEM,
            out_shape=jax.ShapeDtypeStruct((requests, width) if last else partial.shape, bf16),
            cost_estimate=cost(1),
            compiler_params=params(4),
            name="decode_merge",
        )(partial, other)

    def own(ids):
        return pl.pallas_call(
            own_kernel,
            in_specs=[SMEM] + [VMEM] * 4,
            out_specs=[SMEM] + [VMEM] * 4,
            out_shape=[
                jax.ShapeDtypeStruct((DOCS - 1 + heads,), i32),
                *state,
                jax.ShapeDtypeStruct((tiles, 2 * width, tq), bf16),
            ],
            scratch_shapes=pair,
            cost_estimate=cost(3),
            compiler_params=params(16),
            name="prompt_own",
        )(*hbm(head_window, ids.reshape(-1, LANES), prefill_query, prefill_key, prefill_value))

    def far(info, queries, carry, stage, last):
        operands = [x for d in stage for x in (keys[d], values[d])]
        scratch = [pltpu.VMEM((len(stage), kv, tall, tokens), bf16)] + pair
        return pl.pallas_call(
            lambda *refs: far_kernel(*refs, sources=stage, last=last),
            in_specs=[SMEM] + [VMEM] * (4 + len(operands)),
            out_specs=[VMEM] * (3 + last),
            out_shape=state + [jax.ShapeDtypeStruct((tokens, width), bf16)] * last,
            input_output_aliases={2: 0, 3: 1, 4: 2},
            scratch_shapes=scratch,
            cost_estimate=cost(5),
            compiler_params=params(20),
            name="prompt_far",
        )(info, queries, *carry, *operands)

    token = [()]

    def then(x):
        x, *token[0] = lax.optimization_barrier((x, *token[0]))
        return x

    def done(*values):
        token[0] = list(values)
        return values if len(values) > 1 else values[0]

    keys, values = {0: prefill_key}, {0: prefill_value}

    def relay(table, d):
        table[d] = done(then(table[d]))
        if d < reach:
            table[d + 2] = ring(table[d], 2)
        fresh = done(pick(table[d - 2], table[d]))
        table[d - 1] = swap(fresh)

    keys[2] = ring(prefill_key, 2)
    partial = done(decode_pages(page_order))
    other = swap(partial)
    values[2] = ring(prefill_value, 2)
    relay(keys, 2)
    info, *carry, queries = done(*own(then(doc_ids)))
    relay(values, 2)
    bit = 2

    def step(partial, other, bit):
        partial = done(merge(then(partial), other, bit >= n))
        if bit >= n:
            return partial, None, bit
        return partial, swap(partial, bit), bit * 2

    def attend(*stage):
        carry[0] = then(carry[0])
        carry[:] = far(info, queries, carry[:3], stage, stage[-1] == reach - 1)
        done(carry[0])

    partial, other, bit = step(partial, other, bit)
    for d in range(4, reach + 1, 2):
        relay(keys, d)
        attend(d - 2)
        relay(values, d)
        if bit < n:
            partial, other, bit = step(partial, other, bit)
        attend(d - 3)
    attend(reach, reach - 1)
    while other is not None:
        partial, other, bit = step(partial, other, bit)
    attn, decode_attn = carry[-1], partial

    model = out_proj.shape[1]
    tr, dr = tokens // 2, requests // 2
    chunks = 2
    cols = model // chunks

    def project(column, second):
        return pl.pallas_call(
            lambda *refs: project_kernel(*refs, column=column, second=second),
            in_specs=[VMEM] * 3,
            out_specs=VMEM,
            out_shape=jax.ShapeDtypeStruct((tr + dr, cols), bf16),
            cost_estimate=cost(2),
            compiler_params=params(16),
            name="project_own" if second else "project_theirs",
        )(attn, decode_attn, out_proj)

    received = []
    for c in range(chunks):
        sent = project(c * cols, 0)
        received.append(lax.ppermute(sent, "tp", [(0, 1), (1, 0)]))
        decode_attn = lax.optimization_barrier((decode_attn, sent))[0]
    outs = [jax.ShapeDtypeStruct((tr, model), bf16), jax.ShapeDtypeStruct((dr, model), bf16)]
    anywhere = [pl.BlockSpec(memory_space=pl.ANY)] * 2
    buffers = [pltpu.VMEM((tr + dr, cols), bf16), pltpu.SemaphoreType.DMA((4,))]
    mine = project(0, 1)
    *outputs, mine = pl.pallas_call(
        early_kernel,
        in_specs=[VMEM] * 5,
        out_specs=anywhere + [VMEM],
        out_shape=outs + [jax.ShapeDtypeStruct((tr + dr, cols), bf16)],
        scratch_shapes=buffers,
        cost_estimate=cost(2),
        compiler_params=params(16),
        name="project_early",
    )(attn, decode_attn, out_proj, mine, received[0])
    return tuple(
        pl.pallas_call(
            late_kernel,
            in_specs=[VMEM] * 2 + anywhere,
            out_specs=anywhere,
            out_shape=outs,
            input_output_aliases={2: 0, 3: 1},
            scratch_shapes=buffers,
            cost_estimate=cost(1),
            compiler_params=params(8),
            name="project_late",
        )(mine, received[1], *outputs)
    )


def solution(mesh):
    placed = (
        P(("rep", "seq"), "tp"),
        P(("rep", "seq"), "tp"),
        P(("rep", "seq"), "tp"),
        P("rep"),
        P("tp"),
        P("rep", "tp"),
        P("rep", "tp"),
        P("rep", "tp"),
        P(("rep", "seq"), "tp"),
        P(("rep", "seq"), "tp"),
        P(("rep", "seq")),
        P("rep"),
        P("tp", None),
    )

    return jax.shard_map(
        on_device,
        mesh=mesh,
        in_specs=placed,
        out_specs=(P(("rep", "seq", "tp"), None), P(("rep", "tp"), None)),
        check_vma=False,
    )
```
